16 devices in a mesh: fsdp: 16 (over z, y, x, core).
Axes of the slice: x: 2, y: 2, z: 2, core: 2. Of those that a mesh axis runs over, the one named last changes fastest.
Arguments:
- tok_ids: int32 [16384], P('fsdp')
- tok_labels: int32 [16384], P('fsdp')
- loss_mask: int32 [16384], P('fsdp')
- emb_table: bfloat16 [57344, 256], P('fsdp')
- gain_mlp: float32 [256], replicated
- gain_head: float32 [256], replicated
- w_gate: bfloat16 [256, 1536], P('fsdp')
- w_up: bfloat16 [256, 1536], P('fsdp')
- w_down: bfloat16 [1536, 256], P('fsdp')
Outputs:
- output 1: float32 [], replicated
- output 2: float32 [57344, 256], P('fsdp')
- output 3: float32 [256, 1536], P('fsdp')
- output 4: float32 [256, 1536], P('fsdp')
- output 5: float32 [1536, 256], P('fsdp')
All inputs are finite; a program needn't handle non-finite values.
Results may differ from the reference program's by a relative error of at most 0.00885336.
Values are sent between devices in bfloat16 or wider.
A program may use at most 1 GiB of HBM per device.

```python
import jax
import jax.numpy as jnp
from jax import lax

VOCAB = 57344
D_MODEL = 256
D_FF = 1536
TOK_DEV = 1024
GROUP_SIZE = 16
T_GLOBAL = TOK_DEV * GROUP_SIZE
NORM_EPS = 1e-6
ROW_CONTRACT = (((1,), (1,)), ((), ()))
TOK_CONTRACT = (((0,), (0,)), ((), ()))


def draw_tokens(tok_key):
    key_ids, key_lab, key_pad, key_cut = jax.random.split(tok_key, 4)
    tok_ids = jax.random.randint(key_ids, (T_GLOBAL,), 0, VOCAB, dtype=jnp.int32)
    tok_ids = tok_ids.at[0].set(0).at[1].set(VOCAB - 1)
    tok_labels = jax.random.randint(key_lab, (T_GLOBAL,), 0, VOCAB, dtype=jnp.int32)
    tok_labels = tok_labels.at[0].set(VOCAB - 1).at[1].set(0)
    pad_len = jax.random.randint(key_pad, (GROUP_SIZE, 1), 0, TOK_DEV // 2 + 1, dtype=jnp.int32)
    keep_tail = jnp.arange(TOK_DEV)[None, :] < TOK_DEV - pad_len
    cut_draw = jax.random.randint(key_cut, (GROUP_SIZE, TOK_DEV), 0, 16, dtype=jnp.int32)
    loss_mask = (keep_tail & (cut_draw != 0)).astype(jnp.int32).reshape(T_GLOBAL)
    return tok_ids, tok_labels, loss_mask.at[0].set(1)


def setup_inputs(seed: int = 0) -> dict:
    root_key = jax.random.key(seed)
    key_tok, key_emb, key_g1, key_g2, key_gate, key_up, key_down = jax.random.split(root_key, 7)
    tok_ids, tok_labels, loss_mask = draw_tokens(key_tok)
    emb_table = (jax.random.normal(key_emb, (VOCAB, D_MODEL), jnp.float32) * D_MODEL ** -0.5).astype(jnp.bfloat16)
    gain_mlp = 1.0 + 0.5 * jax.random.normal(key_g1, (D_MODEL,), jnp.float32)
    gain_head = 1.0 + 0.5 * jax.random.normal(key_g2, (D_MODEL,), jnp.float32)
    w_gate = (jax.random.normal(key_gate, (D_MODEL, D_FF), jnp.float32) * D_MODEL ** -0.5).astype(jnp.bfloat16)
    w_up = (jax.random.normal(key_up, (D_MODEL, D_FF), jnp.float32) * D_MODEL ** -0.5).astype(jnp.bfloat16)
    w_down = (jax.random.normal(key_down, (D_FF, D_MODEL), jnp.float32) * 1.5 * (D_FF * D_MODEL) ** -0.5).astype(jnp.bfloat16)
    return {"tok_ids": tok_ids, "tok_labels": tok_labels, "loss_mask": loss_mask, "emb_table": emb_table, "gain_mlp": gain_mlp, "gain_head": gain_head, "w_gate": w_gate, "w_up": w_up, "w_down": w_down}


def rms_scale(rows_wide, norm_gain):
    inv_rms = lax.rsqrt(jnp.mean(rows_wide * rows_wide, axis=-1, keepdims=True) + NORM_EPS)
    return (rows_wide * inv_rms * norm_gain).astype(jnp.bfloat16), inv_rms


def rms_back(rows_wide, inv_rms, norm_gain, grad_out):
    scaled_grad = grad_out * norm_gain
    return inv_rms * (scaled_grad - rows_wide * (inv_rms * inv_rms) * jnp.mean(scaled_grad * rows_wide, axis=-1, keepdims=True))


def mlp_forward(emb_rows, gain_mlp, gain_head, w_gate, w_up, w_down):
    emb_wide = emb_rows.astype(jnp.float32)
    a_norm, inv_first = rms_scale(emb_wide, gain_mlp)
    gate_wide = jnp.dot(a_norm, w_gate, preferred_element_type=jnp.float32).astype(jnp.bfloat16).astype(jnp.float32)
    up_wide = jnp.dot(a_norm, w_up, preferred_element_type=jnp.float32).astype(jnp.bfloat16).astype(jnp.float32)
    gate_sig = jax.nn.sigmoid(gate_wide)
    act_rows = (gate_wide * gate_sig * up_wide).astype(jnp.bfloat16)
    hid_wide = (emb_wide + jnp.dot(act_rows, w_down, preferred_element_type=jnp.float32)).astype(jnp.bfloat16).astype(jnp.float32)
    h_norm, inv_second = rms_scale(hid_wide, gain_head)
    return (emb_wide, inv_first, a_norm, gate_wide, up_wide, gate_sig, act_rows, hid_wide, inv_second), h_norm


def head_forward(h_norm, emb_table, tok_labels, tok_coef):
    logits = lax.dot_general(h_norm, emb_table, ROW_CONTRACT, preferred_element_type=jnp.float32)
    row_max = jnp.max(logits, axis=-1, keepdims=True)
    exp_rows = jnp.exp(logits - row_max)
    sum_exp = jnp.sum(exp_rows, axis=-1, keepdims=True)
    is_label = jnp.arange(logits.shape[1])[None, :] == tok_labels[:, None]
    picked = jnp.sum(jnp.where(is_label, logits, 0.0), axis=-1)
    tok_loss = row_max[:, 0] + jnp.log(sum_exp[:, 0]) - picked
    d_logits = ((exp_rows / sum_exp - is_label.astype(jnp.float32)) * tok_coef[:, None]).astype(jnp.bfloat16)
    return jnp.sum(tok_coef * tok_loss), d_logits


def mlp_backward(saved, d_hidden, gain_mlp, w_gate, w_up, w_down):
    emb_wide, inv_first, a_norm, gate_wide, up_wide, gate_sig, act_rows = saved[:7]
    hid_grad = d_hidden.astype(jnp.bfloat16)
    d_act = lax.dot_general(hid_grad, w_down, ROW_CONTRACT, preferred_element_type=jnp.float32)
    grad_down = lax.dot_general(act_rows, hid_grad, TOK_CONTRACT, preferred_element_type=jnp.float32)
    d_up = (d_act * gate_wide * gate_sig).astype(jnp.bfloat16)
    d_gate = (d_act * up_wide * gate_sig * (1.0 + gate_wide * (1.0 - gate_sig))).astype(jnp.bfloat16)
    grad_gate = lax.dot_general(a_norm, d_gate, TOK_CONTRACT, preferred_element_type=jnp.float32)
    grad_up = lax.dot_general(a_norm, d_up, TOK_CONTRACT, preferred_element_type=jnp.float32)
    d_anorm = lax.dot_general(d_gate, w_gate, ROW_CONTRACT, preferred_element_type=jnp.float32) + lax.dot_general(d_up, w_up, ROW_CONTRACT, preferred_element_type=jnp.float32)
    grad_x = d_hidden + rms_back(emb_wide, inv_first, gain_mlp, d_anorm)
    return grad_x, grad_gate, grad_up, grad_down


def block_grads(tok_ids, tok_labels, tok_coef, emb_table, gain_mlp, gain_head, w_gate, w_up, w_down):
    saved, h_norm = mlp_forward(jnp.take(emb_table, tok_ids, axis=0), gain_mlp, gain_head, w_gate, w_up, w_down)
    loss_part, d_logits = head_forward(h_norm, emb_table, tok_labels, tok_coef)
    d_hnorm = jnp.dot(d_logits, emb_table, preferred_element_type=jnp.float32)
    head_grad = lax.dot_general(d_logits, h_norm, TOK_CONTRACT, preferred_element_type=jnp.float32)
    d_hidden = rms_back(saved[7], saved[8], gain_head, d_hnorm)
    grad_x, grad_gate, grad_up, grad_down = mlp_backward(saved, d_hidden, gain_mlp, w_gate, w_up, w_down)
    grad_table = head_grad + jax.ops.segment_sum(grad_x, tok_ids, num_segments=emb_table.shape[0])
    return loss_part, grad_table, grad_gate, grad_up, grad_down


def reference(tok_ids, tok_labels, loss_mask, emb_table, gain_mlp, gain_head, w_gate, w_up, w_down):
    mask_wide = loss_mask.astype(jnp.float32)
    tok_coef = (mask_wide / jnp.sum(mask_wide)).reshape(GROUP_SIZE, TOK_DEV)

    def scan_step(acc_state, block_in):
        step_out = block_grads(block_in[0], block_in[1], block_in[2], emb_table, gain_mlp, gain_head, w_gate, w_up, w_down)
        return tuple(prev_val + new_val for prev_val, new_val in zip(acc_state, step_out)), None

    init_state = (jnp.zeros((), jnp.float32), jnp.zeros((VOCAB, D_MODEL), jnp.float32), jnp.zeros((D_MODEL, D_FF), jnp.float32), jnp.zeros((D_MODEL, D_FF), jnp.float32), jnp.zeros((D_FF, D_MODEL), jnp.float32))
    blocks = (tok_ids.reshape(GROUP_SIZE, TOK_DEV), tok_labels.reshape(GROUP_SIZE, TOK_DEV), tok_coef)
    final_state, _ = lax.scan(scan_step, init_state, blocks)
    loss_val, grad_table, grad_gate, grad_up, grad_down = final_state
    return (loss_val, grad_table, grad_gate, grad_up, grad_down)
```

```python
import functools

import jax
import jax.numpy as jnp
from jax import lax
from jax.experimental import pallas as pl
from jax.experimental.pallas import tpu as pltpu
from jax.sharding import PartitionSpec as P

NORM_EPS = 1e-6
ROW_CONTRACT = (((1,), (1,)), ((), ()))
TOK_CONTRACT = (((0,), (0,)), ((), ()))
MESH = pl.DeviceIdType.MESH
F32 = jnp.float32
BF16 = jnp.bfloat16
LOG2E = 1.4426950408889634
LN2 = 0.6931471805599453

NDEV = 16
NCHIP = 8
ROWS = 3584
TOK = 1024
DIM = 256
FF = 1536
CAP = 96
TV = 512
NT = 512
V_CHIP = 2 * ROWS
NTILE = V_CHIP // TV
NCHUNK = TOK // NT
PER_BLOCK = NTILE * NCHUNK
TOTAL = NCHIP * PER_BLOCK


def flip(chip, mask):
    out = 0
    for bit in (1, 2, 4):
        a, m = lax.rem(lax.div(chip, bit), 2), lax.rem(lax.div(mask, bit), 2)
        out = out + (a + m - 2 * a * m) * bit
    return out


def barrier_all(me):
    bar = pltpu.get_barrier_semaphore()
    for k in range(1, NDEV):
        pl.semaphore_signal(bar, inc=1, device_id=(lax.rem(me + k, NDEV),), device_id_type=MESH)
    pl.semaphore_wait(bar, NDEV - 1)


def params(cid, mib):
    return pltpu.CompilerParams(collective_id=cid, has_side_effects=True, vmem_limit_bytes=mib * 2**20)


VMEM_SPEC = pl.BlockSpec(memory_space=pltpu.VMEM)


def gather_kernel(meta, gate, up, down, meta_o, gate_o, up_o, down_o, ms, mr, ws, wr, fs, fr):
    me = lax.axis_index("fsdp")
    chip, core = lax.div(me, 2), lax.rem(me, 2)
    partner = 2 * chip + 1 - core
    barrier_all(me)
    sends = []
    for k in range(1, NDEV):
        other = lax.rem(me + k, NDEV)
        cp = pltpu.make_async_remote_copy(meta, meta_o.at[me], ms.at[k], mr.at[me], device_id=(other,), device_id_type=MESH)
        cp.start()
        sends.append(cp)
    srcs, outs = (gate, up, down), (gate_o, up_o, down_o)
    for mask in range(1, NCHIP):
        other = 2 * flip(chip, mask) + core
        for i in range(3):
            cp = pltpu.make_async_remote_copy(srcs[i], outs[i].at[me], ws.at[i, mask], wr.at[i, chip], device_id=(other,), device_id_type=MESH)
            cp.start()
            sends.append(cp)
    for i in range(3):
        cp = pltpu.make_async_remote_copy(srcs[i], outs[i].at[me], fs.at[i, chip], fr.at[i, chip], device_id=(partner,), device_id_type=MESH)
        cp.start()
        sends.append(cp)
        outs[i][me] = srcs[i][...]
    meta_o[me] = meta[...]
    for mask in range(1, NCHIP):
        there = flip(chip, mask)
        slot = 2 * there + core
        for i in range(3):
            pltpu.make_async_remote_copy(srcs[i], outs[i].at[slot], ws.at[i, mask], wr.at[i, there], device_id=(partner,), device_id_type=MESH).wait_recv()
            cp = pltpu.make_async_remote_copy(outs[i].at[slot], outs[i].at[slot], fs.at[i, there], fr.at[i, there], device_id=(partner,), device_id_type=MESH)
            cp.start()
            sends.append(cp)
    for k in range(1, NDEV):
        other = lax.rem(me + k, NDEV)
        pltpu.make_async_remote_copy(meta, meta_o.at[other], ms.at[k], mr.at[other], device_id=(other,), device_id_type=MESH).wait_recv()
    for mask in range(NCHIP):
        there = flip(chip, mask)
        for i in range(3):
            pltpu.make_async_remote_copy(srcs[i], outs[i].at[2 * there + 1 - core], fs.at[i, there], fr.at[i, there], device_id=(partner,), device_id_type=MESH).wait_recv()
    for cp in sends:
        cp.wait_send()


def gather_small(meta, gate, up, down):
    dma = pltpu.SemaphoreType.DMA
    return pl.pallas_call(
        gather_kernel,
        name="gather_small",
        out_shape=[jax.ShapeDtypeStruct((NDEV,) + a.shape, a.dtype) for a in (meta, gate, up, down)],
        in_specs=[VMEM_SPEC] * 4,
        out_specs=[VMEM_SPEC] * 4,
        scratch_shapes=[dma((NDEV,)), dma((NDEV,)), dma((3, NCHIP)), dma((3, NCHIP)), dma((3, NCHIP)), dma((3, NCHIP))],
        compiler_params=params(0, 24),
    )(meta, gate, up, down)


def send_blocks(me, send, recv, ss, rs):
    def start(k, carry):
        other = lax.rem(me + k, NDEV)
        pltpu.make_async_remote_copy(send.at[other], recv.at[me], ss.at[other], rs.at[me], device_id=(other,), device_id_type=MESH).start()
        return carry

    lax.fori_loop(1, NDEV, start, 0)


def wait_blocks(me, send, recv, ss, rs):
    def wait(k, carry):
        other = lax.rem(me + k, NDEV)
        pltpu.make_async_remote_copy(send.at[other], recv.at[other], ss.at[other], rs.at[other], device_id=(other,), device_id_type=MESH).wait()
        return carry

    lax.fori_loop(1, NDEV, wait, 0)


def rows_kernel(keys, lids, table, recv, local, send, ss, rs):
    me = lax.axis_index("fsdp")
    barrier_all(me)
    slot_iota = lax.broadcasted_iota(jnp.int32, (CAP, TOK), 0)
    for d in range(NDEV):
        hit = keys[d : d + 1, :] == slot_iota
        local[d] = jnp.sum(jnp.where(hit, lids[d : d + 1, :] + 1, 0).astype(F32), axis=1, keepdims=True)

    group = 4
    row_iota = lax.broadcasted_iota(jnp.int32, (group * CAP, 256), 1)

    def pack(g, carry):
        col = jnp.concatenate([local[g * group + j] for j in range(group)], axis=0).astype(jnp.int32)
        acc = jnp.zeros((group * CAP, DIM), F32)
        for v in range(ROWS // 256):
            pick = jnp.where(row_iota + (v * 256 + 1) == col, 1.0, 0.0).astype(BF16)
            acc = acc + jnp.dot(pick, table[v * 256 : (v + 1) * 256, :], preferred_element_type=F32)
        rows = acc.astype(BF16)
        for j in range(group):
            send[g * group + j] = rows[j * CAP : (j + 1) * CAP]
        return carry

    lax.fori_loop(0, NDEV // group, pack, 0)
    send_blocks(me, send, recv, ss, rs)
    recv[me] = send[me]
    wait_blocks(me, send, recv, ss, rs)


def fetch_rows(keys, lids, table):
    dma = pltpu.SemaphoreType.DMA
    return pl.pallas_call(
        rows_kernel,
        name="fetch_rows",
        out_shape=[jax.ShapeDtypeStruct((NDEV, CAP, DIM), BF16), jax.ShapeDtypeStruct((NDEV, CAP, 1), F32)],
        in_specs=[VMEM_SPEC] * 3,
        out_specs=[VMEM_SPEC] * 2,
        scratch_shapes=[pltpu.VMEM((NDEV, CAP, DIM), BF16), dma((NDEV,)), dma((NDEV,))],
        compiler_params=params(1, 40),
    )(keys, lids, table)


def split3(wide):
    hi = wide.astype(BF16)
    rest = wide - hi.astype(F32)
    mid = rest.astype(BF16)
    return hi, mid, (rest - mid.astype(F32)).astype(BF16)


def grads_kernel(pos, dx, recv, send, parts, ss, rs):
    me = lax.axis_index("fsdp")
    barrier_all(me)
    hi, mid, low = split3(dx[...])
    parts[:, :DIM] = hi
    parts[:, DIM : 2 * DIM] = mid
    parts[:, 2 * DIM :] = low
    slot_iota = lax.broadcasted_iota(jnp.int32, (CAP, TOK), 0)

    def pack(k, carry):
        other = lax.rem(me + k, NDEV)
        pick = jnp.where(pos[0:1, :] - other * CAP == slot_iota, 1.0, 0.0).astype(BF16)
        rows = jnp.dot(pick, parts[...], preferred_element_type=F32)
        send[other] = (rows[:, :DIM] + rows[:, DIM : 2 * DIM]) + rows[:, 2 * DIM :]

        @pl.when(k < NDEV)
        def _():
            pltpu.make_async_remote_copy(send.at[other], recv.at[me], ss.at[other], rs.at[me], device_id=(other,), device_id_type=MESH).start()

        return carry

    lax.fori_loop(1, NDEV + 1, pack, 0)
    recv[me] = send[me]
    wait_blocks(me, send, recv, ss, rs)


def send_grads(pos, dx):
    dma = pltpu.SemaphoreType.DMA
    return pl.pallas_call(
        grads_kernel,
        name="send_grads",
        out_shape=jax.ShapeDtypeStruct((NDEV, CAP, DIM), F32),
        in_specs=[VMEM_SPEC] * 2,
        out_specs=VMEM_SPEC,
        scratch_shapes=[pltpu.VMEM((NDEV, CAP, DIM), F32), pltpu.VMEM((TOK, 3 * DIM), BF16), dma((NDEV,)), dma((NDEV,))],
        compiler_params=params(2, 40),
    )(pos, dx)


def add_kernel(local, rows, base, out, parts):
    @pl.when(pl.program_id(0) == 0)
    def _():
        hi, mid, low = split3(rows[...])
        parts[:, :DIM] = hi
        parts[:, DIM : 2 * DIM] = mid
        parts[:, 2 * DIM :] = low

    first = pl.program_id(0) * 256 + 1
    iota = lax.broadcasted_iota(jnp.int32, (256, NDEV * CAP), 0) + first
    pick = jnp.where(iota == local[...], 1.0, 0.0).astype(BF16)
    sums = jnp.dot(pick, parts[...], preferred_element_type=F32)
    out[...] = base[...] + ((sums[:, :DIM] + sums[:, DIM : 2 * DIM]) + sums[:, 2 * DIM :])


def add_rows(local, rows, base):
    n = NDEV * CAP
    return pl.pallas_call(
        add_kernel,
        name="add_rows",
        grid=(ROWS // 256,),
        out_shape=jax.ShapeDtypeStruct((ROWS, DIM), F32),
        in_specs=[pl.BlockSpec((1, n), lambda i: (0, 0)), pl.BlockSpec((n, DIM), lambda i: (0, 0)), pl.BlockSpec((256, DIM), lambda i: (i, 0))],
        out_specs=pl.BlockSpec((256, DIM), lambda i: (i, 0)),
        scratch_shapes=[pltpu.VMEM((n, 3 * DIM), BF16)],
        compiler_params=pltpu.CompilerParams(vmem_limit_bytes=40 * 2**20),
    )(local.reshape(1, n).astype(jnp.int32), rows.reshape(n, DIM), base)


def reduce_kernel(gate, up, down, loss, gate_o, up_o, down_o, loss_o, pg, pu, pd, sg, su, sd, rg, ru, rd, ls, ps, pr, ss, rs, lss, lrs):
    me = lax.axis_index("fsdp")
    chip, core = lax.div(me, 2), lax.rem(me, 2)
    partner = 2 * chip + 1 - core
    barrier_all(me)
    srcs, pairs, sums, recvs, outs = (gate, up, down), (pg, pu, pd), (sg, su, sd), (rg, ru, rd), (gate_o, up_o, down_o)
    sends = []
    for i in range(3):
        cp = pltpu.make_async_remote_copy(srcs[i].at[1 - core], pairs[i], ps.at[i], pr.at[i], device_id=(partner,), device_id_type=MESH)
        cp.start()
        sends.append(cp)
    for k in range(1, NDEV):
        cp = pltpu.make_async_remote_copy(loss, ls.at[me], lss.at[k], lrs.at[me], device_id=(lax.rem(me + k, NDEV),), device_id_type=MESH)
        cp.start()
        sends.append(cp)
    ls[me] = loss[...]
    for i in range(3):
        pltpu.make_async_remote_copy(srcs[i].at[1 - core], pairs[i], ps.at[i], pr.at[i], device_id=(partner,), device_id_type=MESH).wait_recv()
        sums[i][...] = srcs[i][core] + pairs[i][...]
        for mask in range(NCHIP - 1, 0, -1):
            there = flip(chip, mask)
            cp = pltpu.make_async_remote_copy(sums[i].at[there], recvs[i].at[chip], ss.at[i, mask], rs.at[i, chip], device_id=(2 * there + core,), device_id_type=MESH)
            cp.start()
            sends.append(cp)
        recvs[i][chip] = sums[i][chip]
    for i in range(3):
        for mask in range(1, NCHIP):
            there = flip(chip, mask)
            pltpu.make_async_remote_copy(sums[i].at[there], recvs[i].at[there], ss.at[i, mask], rs.at[i, there], device_id=(2 * there + core,), device_id_type=MESH).wait_recv()
        outs[i][...] = jnp.sum(recvs[i][...], axis=0)
    for k in range(1, NDEV):
        other = lax.rem(me + k, NDEV)
        pltpu.make_async_remote_copy(loss, ls.at[other], lss.at[k], lrs.at[other], device_id=(other,), device_id_type=MESH).wait_recv()
    loss_o[...] = jnp.sum(ls[...], axis=0)
    for cp in sends:
        cp.wait_send()


def reduce_weights(gate, up, down, loss):
    dma = pltpu.SemaphoreType.DMA
    big = (gate, up, down)
    return pl.pallas_call(
        reduce_kernel,
        name="reduce_weights",
        out_shape=[jax.ShapeDtypeStruct(a.shape[2:], F32) for a in big] + [jax.ShapeDtypeStruct(loss.shape, F32)],
        in_specs=[VMEM_SPEC] * 4,
        out_specs=[VMEM_SPEC] * 4,
        scratch_shapes=[pltpu.VMEM(a.shape[1:], F32) for a in big] * 3
        + [pltpu.VMEM((NDEV,) + loss.shape, F32), dma((3,)), dma((3,)), dma((3, NCHIP)), dma((3, NCHIP)), dma((NDEV,)), dma((NDEV,))],
        compiler_params=params(3, 40),
    )(gate, up, down, loss)


def head_kernel(hn, e_own, lab, coef, dhn_o, de_o, loss_o, hn_all, e_full, e_t, d_e, dhn_buf, dhn_recv, stat, stat_recv, lse_own, lse_all, la, lb, da, db,
                hs, hr, es, er, sts, str_, lss, lsr, ds_, dr, xs, xr):
    me = lax.axis_index("fsdp")
    chip, core = lax.div(me, 2), lax.rem(me, 2)
    partner = 2 * chip + 1 - core
    bar = pltpu.get_barrier_semaphore()
    pl.semaphore_signal(bar, inc=1, device_id=(partner,), device_id_type=MESH)
    for mask in range(1, NCHIP):
        pl.semaphore_signal(bar, inc=1, device_id=(2 * flip(chip, mask) + core,), device_id_type=MESH)
    pl.semaphore_wait(bar, NCHIP)

    def same_core(there):
        return dict(device_id=(2 * there + core,), device_id_type=MESH)

    mine = pl.ds(pl.multiple_of(core * ROWS, ROWS), ROWS)
    theirs = pl.ds(pl.multiple_of((1 - core) * ROWS, ROWS), ROWS)
    e_copy = pltpu.make_async_remote_copy(e_own, e_full.at[mine], es, er, device_id=(partner,), device_id_type=MESH)
    e_copy.start()

    def hn_copy(there, slot):
        return pltpu.make_async_remote_copy(hn, hn_all.at[slot], hs.at[there], hr.at[slot], **same_core(there))

    for mask in range(1, NCHIP):
        hn_copy(flip(chip, mask), chip).start()
    e_full[mine, :] = e_own[...]
    hn_all[chip] = hn[...]
    pltpu.make_async_remote_copy(e_own, e_full.at[theirs], es, er, device_id=(partner,), device_id_type=MESH).wait()

    def where_is(g, last):
        k = lax.div(g, PER_BLOCK)
        rest = lax.rem(g, PER_BLOCK)
        n, t = lax.div(rest, NTILE), lax.rem(rest, NTILE)
        return k, flip(chip, 7 - k if last else k), pl.multiple_of(n * NT, NT), t

    def logits(g, last, out):
        _, b, n0, t = where_is(g, last)
        out[...] = lax.dot_general(e_full[pl.ds(pl.multiple_of(t * TV, TV), TV), :], hn_all[b, pl.ds(n0, NT), :], ROW_CONTRACT, preferred_element_type=F32)


    def update(tile, first, m, s):
        m = jnp.where(first, -jnp.inf, m)
        top = m
        for r in range(TV // 8):
            top = jnp.maximum(top, tile[8 * r : 8 * r + 8, :] * LOG2E)
        s = jnp.where(first, 0.0, s) * jnp.exp2(m - top)
        for r in range(TV // 8):
            s = s + jnp.exp2(tile[8 * r : 8 * r + 8, :] * LOG2E - top)
        return top, s

    logits(0, False, la)

    def pass1(i, carry):
        m, s = carry
        g = 2 * i
        _, b, n0, t = where_is(g, False)
        logits(g + 1, False, lb)
        m, s = update(la, t == 0, m, s)
        nxt = jnp.minimum(g + 2, TOTAL - 2)

        @pl.when((lax.rem(g + 2, PER_BLOCK) == 0) & (g + 2 < TOTAL))
        def _():
            _, bn, _, _ = where_is(nxt, False)
            hn_copy(bn, bn).wait_recv()

        logits(nxt, False, la)
        m, s = update(lb, False, m, s)

        @pl.when(t == NTILE - 2)
        def _():
            top = jnp.max(m, axis=0, keepdims=True)
            tot = jnp.sum(s * jnp.exp2(m - top), axis=0, keepdims=True)
            stat[b, :, pl.ds(n0, NT)] = top + jnp.log(tot) * LOG2E

        @pl.when((lax.rem(g + 2, PER_BLOCK) == 0) & (g >= PER_BLOCK))
        def _():
            pltpu.make_async_remote_copy(stat.at[b], stat_recv.at[chip], sts.at[b], str_.at[chip], **same_core(b)).start()

        return m, s

    zero = jnp.zeros((8, NT), F32)
    lax.fori_loop(0, TOTAL // 2, pass1, (zero, zero))

    stat_recv[chip] = stat[chip]

    def clear_de(i, carry):
        d_e[pl.ds(pl.multiple_of(i * 256, 256), 256), :] = jnp.zeros((256, DIM), F32)
        e_t[:, pl.ds(pl.multiple_of(i * 256, 256), 256)] = e_full[pl.ds(pl.multiple_of(i * 256, 256), 256), :].T
        return carry

    def clear_dhn(i, carry):
        dhn_buf[i] = jnp.zeros((DIM, TOK), F32)
        return carry

    for mask in range(1, NCHIP):
        there = flip(chip, mask)
        pltpu.make_async_remote_copy(stat.at[there], stat_recv.at[there], sts.at[there], str_.at[there], **same_core(there)).wait_recv()
    stats = stat_recv[...]
    top = jnp.max(stats, axis=0)
    lse_own[...] = top + jnp.log(jnp.sum(jnp.exp2(stats - top[None]), axis=0)) * LOG2E

    def lse_copy(there, slot):
        return pltpu.make_async_remote_copy(lse_own, lse_all.at[slot], lss.at[there], lsr.at[slot], **same_core(there))

    for mask in range(1, NCHIP):
        lse_copy(flip(chip, mask), chip).start()
    lse_all[chip] = lse_own[...]
    lax.fori_loop(0, V_CHIP // 256, clear_de, 0)
    lax.fori_loop(0, NCHIP, clear_dhn, 0)
    for mask in range(1, NCHIP):
        there = flip(chip, mask)
        lse_copy(there, there).wait_recv()

    iota = lax.broadcasted_iota(jnp.int32, (16, NT), 0)

    def soften(g, tile, out, acc):
        _, b, n0, t = where_is(g, True)
        c = coef[b, :, pl.ds(n0, NT)]
        shift = jnp.where(c > 0.0, lse_all[b, :, pl.ds(n0, NT)] - jnp.log(jnp.where(c > 0.0, c, 1.0)) * LOG2E, jnp.inf)
        where = lab[b, :, pl.ds(n0, NT)] - t * TV
        c = jnp.broadcast_to(c, (16, NT))
        shift = jnp.broadcast_to(shift, (16, NT))
        where = jnp.broadcast_to(where, (16, NT))
        for r in range(TV // 16):
            x = tile[16 * r : 16 * r + 16, :]
            w = jnp.where(iota + 16 * r == where, c, 0.0)
            out[16 * r : 16 * r + 16, :] = (jnp.exp2(x * LOG2E - shift) - w).astype(BF16)
            y = w * x
            acc = acc + (y[:8] + y[8:])
        return acc

    def products(g, d):
        k, b, n0, t = where_is(g, True)
        rows = pl.ds(pl.multiple_of(t * TV, TV), TV)
        d_e[rows, :] += jnp.dot(d[...], hn_all[b, pl.ds(n0, NT), :], preferred_element_type=F32)
        dhn_buf[k, :, pl.ds(n0, NT)] += jnp.dot(e_t[:, rows], d[...], preferred_element_type=F32)

    def dhn_copy(k, there, slot):
        return pltpu.make_async_remote_copy(dhn_buf.at[k], dhn_recv.at[slot], ds_.at[k], dr.at[slot], **same_core(there))

    logits(0, True, la)
    logits(1, True, lb)
    picked = soften(0, la, da, zero)

    def pass2(i, picked):
        g = 2 * i
        logits(g + 2, True, la)
        picked = soften(g + 1, lb, db, picked)
        products(g, da)
        logits(g + 3, True, lb)
        picked = soften(g + 2, la, da, picked)
        products(g + 1, db)

        @pl.when(lax.rem(g + 2, PER_BLOCK) == 0)
        def _():
            k, b, _, _ = where_is(g, True)
            dhn_copy(k, b, chip).start()

        return picked

    picked = lax.fori_loop(0, TOTAL // 2 - 1, pass2, picked)
    picked = soften(TOTAL - 1, lb, db, picked)
    products(TOTAL - 2, da)
    products(TOTAL - 1, db)

    de_recv = dhn_recv
    del de_recv

    def de_copy(rows):
        return pltpu.make_async_remote_copy(d_e.at[rows], de_o, xs, xr, device_id=(partner,), device_id_type=MESH)

    de_copy(theirs).start()
    own = coef[chip] * lse_own[...] * LN2
    loss_o[...] = jnp.zeros((8, NT), F32) - picked
    for n in range(NCHUNK):
        loss_o[0:1, :] += own[:, n * NT : (n + 1) * NT]
    for mask in range(1, NCHIP):
        there = flip(chip, mask)
        dhn_copy(7 - mask, there, there).wait_recv()
    dhn_recv[chip] = dhn_buf[7]
    total = dhn_recv[0]
    for j in range(1, NCHIP):
        total = total + dhn_recv[j]
    dhn_o[...] = total
    de_copy(theirs).wait()
    de_o[...] += d_e[mine, :]

    for mask in range(1, NCHIP):
        there = flip(chip, mask)
        hn_copy(there, chip).wait_send()
        pltpu.make_async_remote_copy(stat.at[there], stat_recv.at[chip], sts.at[there], str_.at[chip], **same_core(there)).wait_send()
        lse_copy(there, chip).wait_send()
        dhn_copy(7 - mask, there, chip).wait_send()


def head(hn, table, lab, coef):
    dma = pltpu.SemaphoreType.DMA
    vm = pltpu.VMEM
    eight = [dma((NCHIP,)), dma((NCHIP,))]
    one = [dma(()), dma(())]
    return pl.pallas_call(
        head_kernel,
        name="head",
        out_shape=[jax.ShapeDtypeStruct((DIM, TOK), F32), jax.ShapeDtypeStruct((ROWS, DIM), F32), jax.ShapeDtypeStruct((8, NT), F32)],
        in_specs=[VMEM_SPEC] * 4,
        out_specs=[VMEM_SPEC] * 3,
        scratch_shapes=[
            vm((NCHIP, TOK, DIM), BF16), vm((V_CHIP, DIM), BF16), vm((DIM, V_CHIP), BF16), vm((V_CHIP, DIM), F32),
            vm((NCHIP, DIM, TOK), F32), vm((NCHIP, DIM, TOK), F32),
            vm((NCHIP, 1, TOK), F32), vm((NCHIP, 1, TOK), F32), vm((1, TOK), F32), vm((NCHIP, 1, TOK), F32),
            vm((TV, NT), F32), vm((TV, NT), F32), vm((TV, NT), BF16), vm((TV, NT), BF16),
        ]
        + eight + one + eight + eight + eight + one,
        compiler_params=params(4, 63),
    )(hn, table, lab, coef)


def rms_scale(rows_wide, norm_gain):
    inv_rms = lax.rsqrt(jnp.mean(rows_wide * rows_wide, axis=-1, keepdims=True) + NORM_EPS)
    return (rows_wide * inv_rms * norm_gain).astype(BF16), inv_rms


def rms_back(rows_wide, inv_rms, norm_gain, grad_out):
    scaled_grad = grad_out * norm_gain
    return inv_rms * (scaled_grad - rows_wide * (inv_rms * inv_rms) * jnp.mean(scaled_grad * rows_wide, axis=-1, keepdims=True))


def mlp_forward(emb_rows, gain_mlp, gain_head, w_gate, w_up, w_down):
    emb_wide = emb_rows.astype(F32)
    a_norm, inv_first = rms_scale(emb_wide, gain_mlp)
    gate_wide = jnp.dot(a_norm, w_gate, preferred_element_type=F32).astype(BF16).astype(F32)
    up_wide = jnp.dot(a_norm, w_up, preferred_element_type=F32).astype(BF16).astype(F32)
    gate_sig = jax.nn.sigmoid(gate_wide)
    act_rows = (gate_wide * gate_sig * up_wide).astype(BF16)
    hid_wide = (emb_wide + jnp.dot(act_rows, w_down, preferred_element_type=F32)).astype(BF16).astype(F32)
    h_norm, inv_second = rms_scale(hid_wide, gain_head)
    return (emb_wide, inv_first, a_norm, gate_wide, up_wide, gate_sig, act_rows, hid_wide, inv_second), h_norm


def mlp_backward(saved, d_hidden, gain_mlp, w_gate, w_up, w_down):
    emb_wide, inv_first, a_norm, gate_wide, up_wide, gate_sig, act_rows = saved[:7]
    hid_grad = d_hidden.astype(BF16)
    d_act = lax.dot_general(hid_grad, w_down, ROW_CONTRACT, preferred_element_type=F32)
    grad_down = lax.dot_general(act_rows, hid_grad, TOK_CONTRACT, preferred_element_type=F32)
    d_up = (d_act * gate_wide * gate_sig).astype(BF16)
    d_gate = (d_act * up_wide * gate_sig * (1.0 + gate_wide * (1.0 - gate_sig))).astype(BF16)
    grad_gate = lax.dot_general(a_norm, d_gate, TOK_CONTRACT, preferred_element_type=F32)
    grad_up = lax.dot_general(a_norm, d_up, TOK_CONTRACT, preferred_element_type=F32)
    d_anorm = lax.dot_general(d_gate, w_gate, ROW_CONTRACT, preferred_element_type=F32) + lax.dot_general(d_up, w_up, ROW_CONTRACT, preferred_element_type=F32)
    grad_x = d_hidden + rms_back(emb_wide, inv_first, gain_mlp, d_anorm)
    return grad_x, grad_gate, grad_up, grad_down


def solution(mesh):
    def device_step(tok_ids, tok_labels, loss_mask, table, gain_mlp, gain_head, gate_shard, up_shard, down_shard):
        me = lax.axis_index("fsdp")
        chip, core = me // 2, me % 2
        meta = jnp.concatenate([tok_ids[None], tok_labels[None], loss_mask[None], jnp.zeros((5, TOK), jnp.int32)], axis=0)
        meta_all, gate_full, up_full, down_full = gather_small(meta, gate_shard, up_shard, down_shard)
        gate_full, up_full, down_full = gate_full.reshape(DIM, FF), up_full.reshape(DIM, FF), down_full.reshape(FF, DIM)
        ids_all = meta_all[:, 0]
        blocks = lax.dynamic_index_in_dim(meta_all.reshape(NCHIP, 2, 8, TOK), core, axis=1, keepdims=False)
        lab_rel = (blocks[:, 1] - chip * V_CHIP)[:, None, :]
        coef = blocks[:, 2].astype(F32)[:, None, :] / jnp.sum(meta_all[:, 2]).astype(F32)

        upper = jnp.triu(jnp.ones((TOK, TOK), BF16), 1)
        lids = ids_all - me * ROWS
        owned = (lids >= 0) & (lids < ROWS)
        rank = jnp.dot(owned.astype(BF16), upper, preferred_element_type=F32).astype(jnp.int32)
        key = jnp.where(owned, rank, -1)
        devices = jnp.arange(NDEV, dtype=jnp.int32)
        owner = tok_ids // ROWS
        is_owner = owner[None, :] == devices[:, None]
        my_rank = jnp.sum(jnp.where(is_owner, jnp.dot(is_owner.astype(BF16), upper, preferred_element_type=F32), 0.0), axis=0).astype(jnp.int32)
        counts = jnp.sum(((ids_all // ROWS)[:, None, :] == devices[None, :, None]).astype(jnp.int32), axis=2)
        rounds = (jnp.max(counts) + CAP - 1) // CAP
        slots = jnp.arange(NDEV * CAP, dtype=jnp.int32)

        def place(r):
            slot = my_rank - r * CAP
            return jnp.where((slot >= 0) & (slot < CAP), owner * CAP + slot, -1)

        def fetch(r):
            got, local = fetch_rows(key - r * CAP, lids, table)
            pick = (place(r)[:, None] == slots[None, :]).astype(BF16)
            return jnp.dot(pick, got.reshape(NDEV * CAP, DIM), preferred_element_type=F32).astype(BF16), local

        emb_rows, local = fetch(0)
        emb_rows = lax.fori_loop(1, rounds, lambda r, rows: rows + fetch(r)[0], emb_rows)

        saved, h_norm = mlp_forward(emb_rows, gain_mlp, gain_head, gate_full, up_full, down_full)
        d_hnorm_t, head_grad, loss_part = head(h_norm, table, lab_rel, coef)
        d_hidden = rms_back(saved[7], saved[8], gain_head, d_hnorm_t.T)
        grad_x, grad_gate, grad_up, grad_down = mlp_backward(saved, d_hidden, gain_mlp, gate_full, up_full, down_full)

        grad_table = add_rows(local, send_grads(place(0)[None], grad_x), head_grad)

        def more(r, acc):
            got = send_grads(place(r)[None], grad_x)
            slot_key = key - r * CAP
            hit = slot_key[:, None, :] == jnp.arange(CAP, dtype=jnp.int32)[None, :, None]
            where = jnp.sum(jnp.where(hit, (lids + 1)[:, None, :], 0), axis=2)
            return add_rows(where, got, acc)

        grad_table = lax.fori_loop(1, rounds, more, grad_table)
        shape_in = lambda g, rows: g.reshape(NCHIP, 2, rows, -1).transpose(1, 0, 2, 3)
        out_gate, out_up, out_down, loss = reduce_weights(shape_in(grad_gate, 16), shape_in(grad_up, 16), shape_in(grad_down, 96), loss_part)
        return jnp.sum(loss), grad_table, out_gate, out_up, out_down

    row_spec = P("fsdp", None)
    tok_spec = P("fsdp")
    return jax.shard_map(device_step, mesh=mesh, in_specs=(tok_spec, tok_spec, tok_spec, row_spec, P(), P(), row_spec, row_spec, row_spec), out_specs=(P(), row_spec, row_spec, row_spec, row_spec), check_vma=False)
```

```python
import functools

import jax
import jax.numpy as jnp
from jax import lax
from jax.experimental import pallas as pl
from jax.experimental.pallas import tpu as pltpu
from jax.sharding import PartitionSpec as P

NORM_EPS = 1e-6
ROW_CONTRACT = (((1,), (1,)), ((), ()))
TOK_CONTRACT = (((0,), (0,)), ((), ()))
MESH = pl.DeviceIdType.MESH
F32 = jnp.float32
BF16 = jnp.bfloat16
LOG2E = 1.4426950408889634
LN2 = 0.6931471805599453

NDEV = 16
NCHIP = 8
ROWS = 3584
TOK = 1024
DIM = 256
FF = 1536
CAP = 96
TV = 1024
NT = 512
V_CHIP = 2 * ROWS
NTILE = V_CHIP // TV
NCHUNK = TOK // NT
PER_BLOCK = NTILE * NCHUNK
TOTAL = NCHIP * PER_BLOCK


def flip(chip, mask):
    out = 0
    for bit in (1, 2, 4):
        a, m = lax.rem(lax.div(chip, bit), 2), lax.rem(lax.div(mask, bit), 2)
        out = out + (a + m - 2 * a * m) * bit
    return out


AXES = ((2, 4, 1), (4, 1, 2), (1, 2, 4))
OTHERS = range(1, NDEV)
MASKS = range(1, NCHIP)
COLS = 256
THREE = range(3)
EACH = (3, NCHIP)


def whereabouts():
    me = lax.axis_index("fsdp")
    chip, core = lax.div(me, 2), lax.rem(me, 2)
    return me, chip, core, me + 1 - core - core


def side(chip, bit):
    return lax.rem(lax.div(chip, bit), 2)


def turn(chip, bits):
    out = chip
    for bit in bits:
        out = out + bit * (1 - 2 * side(chip, bit))
    return out


def barrier_greet(me):
    bar = pltpu.get_barrier_semaphore()
    for k in OTHERS:
        pl.semaphore_signal(bar, inc=1, device_id=(lax.rem(me + k, NDEV),), device_id_type=MESH)


def barrier_wait():
    pl.semaphore_wait(pltpu.get_barrier_semaphore(), NDEV - 1)


def barrier_all(me):
    barrier_greet(me)
    barrier_wait()


def params(cid, mib):
    return pltpu.CompilerParams(collective_id=cid, has_side_effects=True, vmem_limit_bytes=mib * 2**20)


VMEM_SPEC = pl.BlockSpec(memory_space=pltpu.VMEM)


def pack_rows(ids_key, ids_local, table, send, local):
    slot_iota = lax.broadcasted_iota(jnp.int32, (CAP, TOK), 0)
    for d in range(NDEV):
        hit = ids_key[d : d + 1, :] == slot_iota
        local[d] = jnp.sum(jnp.where(hit, ids_local[d : d + 1, :] + 1, 0).astype(F32), axis=1, keepdims=True)

    group = 4
    row_iota = lax.broadcasted_iota(jnp.int32, (group * CAP, COLS), 1)

    def pack(g, carry):
        col = jnp.concatenate([local[g * group + j] for j in range(group)], axis=0).astype(jnp.int32)
        acc = jnp.zeros((group * CAP, DIM), F32)
        for v in range(ROWS // COLS):
            pick = jnp.where(row_iota + (v * COLS + 1) == col, 1.0, 0.0).astype(BF16)
            acc = acc + jnp.dot(pick, table[v * COLS : (v + 1) * COLS, :], preferred_element_type=F32)
        rows = acc.astype(BF16)
        for j in range(group):
            send[g * group + j] = rows[j * CAP : (j + 1) * CAP]
        return carry

    lax.fori_loop(0, NDEV // group, pack, 0)


STEP = 256


def forward_again(x, gain_mlp, gain_head, gate, up, down):
    shape = jax.ShapeDtypeStruct
    return pl.pallas_call(
        mlp_rows,
        name="forward_again",
        out_shape=[shape((TOK, DIM), BF16)] * 2,
        in_specs=[VMEM_SPEC] * 6,
        out_specs=[VMEM_SPEC] * 2,
        compiler_params=pltpu.CompilerParams(vmem_limit_bytes=48 * 2**20),
    )(x, gain_mlp, gain_head, gate, up, down)


def wide_weights(gate, up, down):
    return gate[...].reshape(DIM, FF), up[...].reshape(DIM, FF), down[...].reshape(FF, DIM)


def swiglu(a, w_gate, w_up):
    p = jnp.dot(a, w_gate, preferred_element_type=F32).astype(BF16).astype(F32)
    q = jnp.dot(a, w_up, preferred_element_type=F32).astype(BF16).astype(F32)
    sig = jax.nn.sigmoid(p)
    return p, q, sig, (p * sig * q).astype(BF16)


def mlp_rows(x, gain_mlp, gain_head, gate, up, down, h_o, hn_o):
    def some(i, carry):
        rows = pl.ds(pl.multiple_of(i * STEP, STEP), STEP)
        w_gate, w_up, w_down = wide_weights(gate, up, down)
        wide = x[rows, :].astype(F32)
        a = rms_scale(wide, gain_mlp[...])[0]
        u = swiglu(a, w_gate, w_up)[3]
        h = (wide + jnp.dot(u, w_down, preferred_element_type=F32)).astype(BF16)
        h_o[rows, :] = h
        hn_o[rows, :] = rms_scale(h.astype(F32), gain_head[...])[0]
        return carry

    lax.fori_loop(0, TOK // STEP, some, 0)


def make_upper(upper):
    for r in range(TOK // 128):
        rows = lax.broadcasted_iota(jnp.int32, (128, TOK), 0) + 128 * r
        cols = lax.broadcasted_iota(jnp.int32, (128, TOK), 1)
        upper[128 * r : 128 * r + 128, :] = jnp.where(rows < cols, 1.0, 0.0).astype(BF16)


def start_kernel(meta, gate, up, down, table, gain_mlp, gain_head, ids_o, lab_o, coef_o, pos_o, x_o, local, h_o, hn_o, gate_o, up_o, down_o,
                 meta_all, key, lid, upper, send, recv, total, ms, mr, ws, wr, fs, fr, ss, rs):
    me, chip, core, partner = whereabouts()
    barrier_greet(me)
    make_upper(upper)
    barrier_wait()
    sends = []
    for k in OTHERS:
        cp = pltpu.make_async_remote_copy(meta, meta_all.at[me], ms.at[k], mr.at[me], device_id=(lax.rem(me + k, NDEV),), device_id_type=MESH)
        cp.start()
        sends.append(cp)
    srcs, outs = (gate, up, down), (gate_o, up_o, down_o)

    def forward(i, src, slot, there):
        return pltpu.make_async_remote_copy(src, outs[i].at[slot], fs.at[i, there], fr.at[i, there], device_id=(partner,), device_id_type=MESH)

    def hop(i, stage, go):
        axes = AXES[i]
        turns = [()]
        for bit in axes[:stage]:
            turns = turns + [bits + (bit,) for bits in turns]
        across = 2 * turn(chip, axes[stage : stage + 1]) + core
        for n, bits in enumerate(turns):
            slot = len(turns) - 1 + n
            there = turn(chip, bits if go else bits + axes[stage : stage + 1])
            block = outs[i].at[2 * there + core]
            cp = pltpu.make_async_remote_copy(srcs[i] if go and not bits else block, block, ws.at[i, slot], wr.at[i, slot], device_id=(across,), device_id_type=MESH)
            if not go:
                cp.wait_recv()
                cp = forward(i, block, 2 * there + core, there)
            cp.start()
            sends.append(cp)

    for i in THREE:
        hop(i, 0, True)
    for i in THREE:
        cp = forward(i, srcs[i], me, chip)
        cp.start()
        sends.append(cp)
        outs[i][me] = srcs[i][...]
    meta_all[me] = meta[...]
    for k in OTHERS:
        other = lax.rem(me + k, NDEV)
        pltpu.make_async_remote_copy(meta, meta_all.at[other], ms.at[k], mr.at[other], device_id=(other,), device_id_type=MESH).wait_recv()

    for i in THREE:
        hop(i, 0, False)
        hop(i, 1, True)

    for d in range(NDEV):
        ids_o[d : d + 1, :] = meta_all[d, 0]
    lids = ids_o[...] - me * ROWS
    owned = (lids >= 0) & (lids < ROWS)
    rank = jnp.dot(jnp.where(owned, 1.0, 0.0).astype(BF16), upper[...], preferred_element_type=F32).astype(jnp.int32)
    key[...] = jnp.where(owned, rank, -1)
    lid[...] = lids
    with jax.named_scope("s_pack"):
        pack_rows(key, lid, table, send, local)
    send_blocks(me, send, recv, ss, rs)
    for i in THREE:
        hop(i, 1, False)
        hop(i, 2, True)
    recv[me] = send[me]

    count = meta_all[0, 2]
    for d in range(1, NDEV):
        count = count + meta_all[d, 2]
    n_all = jnp.sum(count.astype(F32), axis=1, keepdims=True)
    for j in range(NCHIP):
        lab_o[j] = meta_all[2 * j + core, 1] - chip * V_CHIP
        coef_o[j] = meta_all[2 * j + core, 2].astype(F32) / n_all

    first = lax.broadcasted_iota(jnp.int32, (NDEV, TOK), 0) * ROWS
    mine = meta[0]
    is_owner = (mine >= first) & (mine < first + ROWS)
    rank = jnp.dot(jnp.where(is_owner, 1.0, 0.0).astype(BF16), upper[...], preferred_element_type=F32).astype(jnp.int32)
    slot = jnp.where(is_owner & (rank < CAP), lax.broadcasted_iota(jnp.int32, (NDEV, TOK), 0) * CAP + rank, -1)
    pos_o[...] = jnp.max(slot, axis=0, keepdims=True)

    for i in THREE:
        hop(i, 2, False)
    with jax.named_scope("s_wait"):
        wait_blocks(me, send, recv, ss, rs)
    group = 4
    for g in range(NDEV // group):
        iota = lax.broadcasted_iota(jnp.int32, (group * CAP, TOK), 0) + g * group * CAP
        pick = jnp.where(iota == pos_o[...], 1.0, 0.0).astype(BF16)
        rows = jnp.concatenate([recv[g * group + j] for j in range(group)], axis=0)
        part = lax.dot_general(pick, rows, TOK_CONTRACT, preferred_element_type=F32)
        total[...] = part if g == 0 else total[...] + part
    x_o[...] = total[...].astype(BF16)
    for mask in range(NCHIP):
        there = flip(chip, mask)
        for i in THREE:
            forward(i, srcs[i], 2 * there + 1 - core, there).wait_recv()
    with jax.named_scope("s_mlp"):
        mlp_rows(x_o, gain_mlp, gain_head, gate_o, up_o, down_o, h_o, hn_o)
    for cp in sends:
        cp.wait_send()


def start(meta, gate, up, down, table, gain_mlp, gain_head):
    dma = pltpu.SemaphoreType.DMA
    vm = pltpu.VMEM
    shape = jax.ShapeDtypeStruct
    return pl.pallas_call(
        start_kernel,
        name="start",
        out_shape=[
            shape((NDEV, TOK), jnp.int32), shape((NCHIP, 1, TOK), jnp.int32), shape((NCHIP, 1, TOK), F32), shape((1, TOK), jnp.int32),
            shape((TOK, DIM), BF16), shape((NDEV, CAP, 1), F32),
        ]
        + [shape((TOK, DIM), BF16)] * 2
        + [shape((NDEV,) + a.shape, a.dtype) for a in (gate, up, down)],
        in_specs=[VMEM_SPEC] * 7,
        out_specs=[VMEM_SPEC] * 11,
        scratch_shapes=[
            vm((NDEV, 3, 1, TOK), jnp.int32), vm((NDEV, TOK), jnp.int32), vm((NDEV, TOK), jnp.int32), vm((TOK, TOK), BF16),
            vm((NDEV, CAP, DIM), BF16), vm((NDEV, CAP, DIM), BF16), vm((TOK, DIM), F32),
            dma((NDEV,)), dma((NDEV,)), dma(EACH), dma(EACH), dma(EACH), dma(EACH), dma((NDEV,)), dma((NDEV,)),
        ],
        compiler_params=params(0, 60),
    )(meta, gate, up, down, table, gain_mlp, gain_head)


def send_blocks(me, send, recv, ss, rs):
    def start(k, carry):
        other = lax.rem(me + k, NDEV)
        pltpu.make_async_remote_copy(send.at[other], recv.at[me], ss.at[other], rs.at[me], device_id=(other,), device_id_type=MESH).start()
        return carry

    lax.fori_loop(1, NDEV, start, 0)


def wait_blocks(me, send, recv, ss, rs):
    def wait(k, carry):
        other = lax.rem(me + k, NDEV)
        pltpu.make_async_remote_copy(send.at[other], recv.at[other], ss.at[other], rs.at[other], device_id=(other,), device_id_type=MESH).wait()
        return carry

    lax.fori_loop(1, NDEV, wait, 0)


def rows_kernel(keys, lids, table, recv, local, send, ss, rs):
    me = lax.axis_index("fsdp")
    barrier_all(me)
    pack_rows(keys, lids, table, send, local)
    send_blocks(me, send, recv, ss, rs)
    recv[me] = send[me]
    wait_blocks(me, send, recv, ss, rs)


def fetch_rows(keys, lids, table):
    dma = pltpu.SemaphoreType.DMA
    return pl.pallas_call(
        rows_kernel,
        name="fetch_rows",
        out_shape=[jax.ShapeDtypeStruct((NDEV, CAP, DIM), BF16), jax.ShapeDtypeStruct((NDEV, CAP, 1), F32)],
        in_specs=[VMEM_SPEC] * 3,
        out_specs=[VMEM_SPEC] * 2,
        scratch_shapes=[pltpu.VMEM((NDEV, CAP, DIM), BF16), dma((NDEV,)), dma((NDEV,))],
        compiler_params=params(1, 40),
    )(keys, lids, table)


def split3(wide):
    hi = wide.astype(BF16)
    rest = wide - hi.astype(F32)
    mid = rest.astype(BF16)
    return hi, mid, (rest - mid.astype(F32)).astype(BF16)


def put_parts(parts, rows, wide):
    for n, part in enumerate(split3(wide)):
        parts[rows, n * DIM : (n + 1) * DIM] = part


def add_parts(sums):
    return (sums[:, :DIM] + sums[:, DIM : 2 * DIM]) + sums[:, 2 * DIM :]


def pack_grads(me, pos, dx, send, recv, parts, ss, rs):
    put_parts(parts, slice(None), dx[...])
    slot_iota = lax.broadcasted_iota(jnp.int32, (CAP, TOK), 0)

    def pack(k, carry):
        other = lax.rem(me + k, NDEV)
        pick = jnp.where(pos[0:1, :] - other * CAP == slot_iota, 1.0, 0.0).astype(BF16)
        rows = jnp.dot(pick, parts[...], preferred_element_type=F32)
        send[other] = add_parts(rows)

        @pl.when(k < NDEV)
        def _():
            pltpu.make_async_remote_copy(send.at[other], recv.at[me], ss.at[other], rs.at[me], device_id=(other,), device_id_type=MESH).start()

        return carry

    lax.fori_loop(1, NDEV + 1, pack, 0)


def grads_kernel(pos, dx, recv, send, parts, ss, rs):
    me = lax.axis_index("fsdp")
    barrier_all(me)
    pack_grads(me, pos, dx, send, recv, parts, ss, rs)
    recv[me] = send[me]
    wait_blocks(me, send, recv, ss, rs)


def send_grads(pos, dx):
    dma = pltpu.SemaphoreType.DMA
    return pl.pallas_call(
        grads_kernel,
        name="send_grads",
        out_shape=jax.ShapeDtypeStruct((NDEV, CAP, DIM), F32),
        in_specs=[VMEM_SPEC] * 2,
        out_specs=VMEM_SPEC,
        scratch_shapes=[pltpu.VMEM((NDEV, CAP, DIM), F32), pltpu.VMEM((TOK, 3 * DIM), BF16), dma((NDEV,)), dma((NDEV,))],
        compiler_params=params(2, 40),
    )(pos, dx)


def add_kernel(local, rows, base, out, parts):
    @pl.when(pl.program_id(0) == 0)
    def _():
        put_parts(parts, slice(None), rows[...])

    first = pl.program_id(0) * COLS + 1
    iota = lax.broadcasted_iota(jnp.int32, (COLS, NDEV * CAP), 0) + first
    pick = jnp.where(iota == local[...], 1.0, 0.0).astype(BF16)
    sums = jnp.dot(pick, parts[...], preferred_element_type=F32)
    out[...] = base[...] + add_parts(sums)


def add_rows(local, rows, base):
    n = NDEV * CAP
    return pl.pallas_call(
        add_kernel,
        name="add_rows",
        grid=(ROWS // COLS,),
        out_shape=jax.ShapeDtypeStruct((ROWS, DIM), F32),
        in_specs=[pl.BlockSpec((1, n), lambda i: (0, 0)), pl.BlockSpec((n, DIM), lambda i: (0, 0)), pl.BlockSpec((COLS, DIM), lambda i: (i, 0))],
        out_specs=pl.BlockSpec((COLS, DIM), lambda i: (i, 0)),
        scratch_shapes=[pltpu.VMEM((n, 3 * DIM), BF16)],
        compiler_params=pltpu.CompilerParams(vmem_limit_bytes=40 * 2**20),
    )(local.reshape(1, n).astype(jnp.int32), rows.reshape(n, DIM), base)


def weight_grad(left, right, out):
    grad = lax.dot_general(left[...], right[...], TOK_CONTRACT, preferred_element_type=F32)
    rows = out.shape[2]
    for j in range(NDEV):
        out[j // 2, j % 2] = grad[j * rows : (j + 1) * rows]


def finish_kernel(pos, dhn, x, h, w_gate, w_up, w_down, gain_mlp, gain_head, where, base, loss, table_o, gate_o, up_o, down_o, loss_o, dx,
                  gate, up, down, dhid, dhid_b, a_all, u_all, dgate, dup, send, recv, parts, rparts, pg, pu, pd, sg, su, sd, rg, ru, rd, ls, xs, xr, ps, pr, ss, rs, lss, lrs):
    me, chip, core, partner = whereabouts()
    barrier_greet(me)
    srcs, pairs, sums, recvs, outs = (gate, up, down), (pg, pu, pd), (sg, su, sd), (rg, ru, rd), (gate_o, up_o, down_o)
    sends = []

    def pair(i):
        return pltpu.make_async_remote_copy(srcs[i].at[:, 1 - core], pairs[i], ps.at[i], pr.at[i], device_id=(partner,), device_id_type=MESH)

    def back(n, carry):
        rows = pl.ds(pl.multiple_of(n * STEP, STEP), STEP)
        wide = h[rows, :].astype(F32)
        inv = rms_scale(wide, gain_head[...])[1]
        grad = rms_back(wide, inv, gain_head[...], dhn[:, rows].T)
        dhid[rows, :] = grad
        grad = grad.astype(BF16)
        dhid_b[rows, :] = grad
        a = rms_scale(x[rows, :].astype(F32), gain_mlp[...])[0]
        a_all[rows, :] = a
        g_full, u_full, d_full = wide_weights(w_gate, w_up, w_down)
        p, q, sig, act = swiglu(a, g_full, u_full)
        u_all[rows, :] = act
        dact = lax.dot_general(grad, d_full, ROW_CONTRACT, preferred_element_type=F32)
        dup[rows, :] = (dact * p * sig).astype(BF16)
        dgate[rows, :] = (dact * q * sig * (1.0 + p * (1.0 - sig))).astype(BF16)
        return carry

    with jax.named_scope("f_back"):
        lax.fori_loop(0, TOK // STEP, back, 0)
    def hop(i, stage, go):
        b1, b2, b3 = AXES[i]
        base_1, base_2 = side(chip, b1) * b1, side(chip, b2) * b2
        if stage == 0:
            bit, blocks = b1, [(n, n // 2 * b2 + n % 2 * b3) for n in range(4)]
            lead = 0
        elif stage == 1:
            bit, blocks = b2, [(4 + n, n * b3) for n in range(2)]
            lead = base_1
        else:
            bit, blocks = b3, [(6, 0)]
            lead = base_1 + base_2
        across = 2 * turn(chip, (bit,)) + core
        for slot, rest in blocks:
            out_block = lead + (1 - side(chip, bit)) * bit + rest
            in_block = lead + side(chip, bit) * bit + rest
            cp = pltpu.make_async_remote_copy(sums[i].at[out_block], recvs[i].at[slot], ss.at[i, slot], rs.at[i, slot], device_id=(across,), device_id_type=MESH)
            if go:
                cp.start()
                sends.append(cp)
            elif stage < 2:
                cp.wait_recv()
                sums[i][in_block] = sums[i][in_block] + recvs[i][slot]
            else:
                cp.wait_recv()
                outs[i][...] = sums[i][chip] + recvs[i][slot]

    def merge(i):
        pair(i).wait()
        sums[i][...] = srcs[i][:, core] + pairs[i][...]
        hop(i, 0, True)

    def to_rows(n, carry):
        rows = pl.ds(pl.multiple_of(n * STEP, STEP), STEP)
        da = lax.dot_general(dgate[rows, :], w_gate[...].reshape(DIM, FF), ROW_CONTRACT, preferred_element_type=F32)
        da = da + lax.dot_general(dup[rows, :], w_up[...].reshape(DIM, FF), ROW_CONTRACT, preferred_element_type=F32)
        wide = x[rows, :].astype(F32)
        inv = rms_scale(wide, gain_mlp[...])[1]
        dx[rows, :] = dhid[rows, :] + rms_back(wide, inv, gain_mlp[...], da)
        return carry

    lax.fori_loop(0, TOK // STEP, to_rows, 0)
    with jax.named_scope("f_pack"):
        barrier_wait()
        pack_grads(me, pos, dx, send, recv, parts, xs, xr)
    weight_grad(u_all, dhid_b, down)
    pair(2).start()
    weight_grad(a_all, dgate, gate)
    pair(0).start()
    weight_grad(a_all, dup, up)
    pair(1).start()
    for i in (2, 0, 1):
        merge(i)
    for k in OTHERS:
        cp = pltpu.make_async_remote_copy(loss, ls.at[me], lss.at[k], lrs.at[me], device_id=(lax.rem(me + k, NDEV),), device_id_type=MESH)
        cp.start()
        sends.append(cp)
    ls[me] = loss[...]
    recv[me] = send[me]
    with jax.named_scope("f_wait"):
        wait_blocks(me, send, recv, xs, xr)
    for d in range(NDEV):
        put_parts(rparts, slice(d * CAP, (d + 1) * CAP), recv[d])

    def add(v, carry):
        rows = pl.ds(pl.multiple_of(v * NT, NT), NT)
        iota = lax.broadcasted_iota(jnp.int32, (NT, NDEV * CAP), 0) + (v * NT + 1)
        pick = jnp.where(iota == where[...], 1.0, 0.0).astype(BF16)
        got = jnp.dot(pick, rparts[...], preferred_element_type=F32)
        table_o[rows, :] = base[rows, :] + add_parts(got)
        return carry

    with jax.named_scope("f_add"):
        lax.fori_loop(0, 2, add, 0)
        for stage in (0, 1):
            for i in THREE:
                hop(i, stage, False)
                hop(i, stage + 1, True)
            lax.fori_loop(2 * stage + 2, 2 * stage + 4, add, 0)
        lax.fori_loop(6, ROWS // NT, add, 0)
    for i in THREE:
        hop(i, 2, False)
    for k in OTHERS:
        other = lax.rem(me + k, NDEV)
        pltpu.make_async_remote_copy(loss, ls.at[other], lss.at[k], lrs.at[other], device_id=(other,), device_id_type=MESH).wait_recv()
    loss_o[...] = jnp.sum(ls[...], axis=0)
    for cp in sends:
        cp.wait_send()


def finish(pos, dhn, x, h, gate, up, down, gain_mlp, gain_head, where, base, loss):
    dma = pltpu.SemaphoreType.DMA
    vm = pltpu.VMEM
    big = [jax.ShapeDtypeStruct((NCHIP, 2) + a.shape[1:], F32) for a in (gate, up, down)]
    buffers = [vm((NCHIP,) + a.shape[2:], F32) for a in big]
    back = [vm(a.shape, F32) for a in big] + [vm((TOK, DIM), F32), vm((TOK, DIM), BF16), vm((TOK, DIM), BF16), vm((TOK, FF), BF16), vm((TOK, FF), BF16), vm((TOK, FF), BF16)]
    return pl.pallas_call(
        finish_kernel,
        name="finish",
        out_shape=[jax.ShapeDtypeStruct((ROWS, DIM), F32)] + [jax.ShapeDtypeStruct(a.shape[2:], F32) for a in big] + [jax.ShapeDtypeStruct(loss.shape, F32), jax.ShapeDtypeStruct((TOK, DIM), F32)],
        in_specs=[VMEM_SPEC] * 12,
        out_specs=[VMEM_SPEC] * 6,
        scratch_shapes=back + [vm((NDEV, CAP, DIM), F32), vm((NDEV, CAP, DIM), F32), vm((TOK, 3 * DIM), BF16), vm((NDEV * CAP, 3 * DIM), BF16)]
        + buffers * 3
        + [vm((NDEV,) + loss.shape, F32), dma((NDEV,)), dma((NDEV,)), dma((3,)), dma((3,)), dma(EACH), dma(EACH), dma((NDEV,)), dma((NDEV,))],
        compiler_params=params(3, 63),
    )(pos, dhn, x, h, gate, up, down, gain_mlp, gain_head, where, base, loss)


def head_kernel(hn, e_own, lab, coef, dhn_o, de_o, loss_o, hn_all, e_full, e_t, d_e, dhn_buf, dhn_recv, stat, stat_recv, lse_own, lse_all, la, lb, da, db,
                hs, hr, es, er, sts, str_, lss, lsr, ds_, dr, xs, xr):
    me, chip, core, partner = whereabouts()
    bar = pltpu.get_barrier_semaphore()
    pl.semaphore_signal(bar, inc=1, device_id=(partner,), device_id_type=MESH)
    for mask in MASKS:
        pl.semaphore_signal(bar, inc=1, device_id=(2 * flip(chip, mask) + core,), device_id_type=MESH)
    pl.semaphore_wait(bar, NCHIP)

    def same_core(there):
        return dict(device_id=(2 * there + core,), device_id_type=MESH)

    mine = pl.ds(pl.multiple_of(core * ROWS, ROWS), ROWS)
    theirs = pl.ds(pl.multiple_of((1 - core) * ROWS, ROWS), ROWS)
    e_copy = pltpu.make_async_remote_copy(e_own, e_full.at[mine], es, er, device_id=(partner,), device_id_type=MESH)
    e_copy.start()

    def hn_copy(there, slot):
        return pltpu.make_async_remote_copy(hn, hn_all.at[slot], hs.at[there], hr.at[slot], **same_core(there))

    for mask in MASKS:
        hn_copy(flip(chip, mask), chip).start()
    e_full[mine, :] = e_own[...]
    hn_all[chip] = hn[...]
    pltpu.make_async_remote_copy(e_own, e_full.at[theirs], es, er, device_id=(partner,), device_id_type=MESH).wait()

    def where_is(g, last):
        k = lax.div(g, PER_BLOCK)
        rest = lax.rem(g, PER_BLOCK)
        n, t = lax.div(rest, NTILE), lax.rem(rest, NTILE)
        return k, flip(chip, 7 - k if last else k), pl.multiple_of(n * NT, NT), t

    def logits(g, last, out):
        _, b, n0, t = where_is(g, last)
        out[...] = lax.dot_general(e_full[pl.ds(pl.multiple_of(t * TV, TV), TV), :], hn_all[b, pl.ds(n0, NT), :], ROW_CONTRACT, preferred_element_type=F32)


    def logits_top(g, out):
        _, b, n0, t = where_is(g, False)
        tile = lax.dot_general(e_full[pl.ds(pl.multiple_of(t * TV, TV), TV), :], hn_all[b, pl.ds(n0, NT), :], ROW_CONTRACT, preferred_element_type=F32)
        out[...] = tile
        return jnp.max(tile.reshape(TV // 8, 8, NT), axis=0)

    def update(tile, tile_top, first, m, s):
        m = jnp.where(first, -jnp.inf, m)
        top = jnp.maximum(m, tile_top * LOG2E)
        sums = [jnp.where(first, 0.0, s) * jnp.exp2(m - top)] + [None] * 3
        for r in range(TV // 8):
            e = jnp.exp2(tile[8 * r : 8 * r + 8, :] * LOG2E - top)
            sums[r % 4] = e if sums[r % 4] is None else sums[r % 4] + e
        return top, (sums[0] + sums[1]) + (sums[2] + sums[3])

    def keep(g, m, s):
        _, b, n0, t = where_is(g, False)

        @pl.when(t == NTILE - 1)
        def _():
            top = jnp.max(m, axis=0, keepdims=True)
            tot = jnp.sum(s * jnp.exp2(m - top), axis=0, keepdims=True)
            stat[b, :, pl.ds(n0, NT)] = top + jnp.log(tot) * LOG2E

        @pl.when((lax.rem(g + 1, PER_BLOCK) == 0) & (g >= PER_BLOCK))
        def _():
            pltpu.make_async_remote_copy(stat.at[b], stat_recv.at[chip], sts.at[b], str_.at[chip], **same_core(b)).start()

    def pass1(i, carry):
        m, s, top_a = carry
        g = 2 * i
        nxt = jnp.minimum(g + 2, TOTAL - 2)

        @pl.when((lax.rem(g + 2, PER_BLOCK) == 0) & (g + 2 < TOTAL))
        def _():
            _, bn, _, _ = where_is(nxt, False)
            hn_copy(bn, bn).wait_recv()

        top_b = logits_top(g + 1, lb)
        ma, sa = update(la, top_a, where_is(g, False)[3] == 0, m, s)
        top_a = logits_top(nxt, la)
        mb, sb = update(lb, top_b, where_is(g + 1, False)[3] == 0, ma, sa)
        keep(g, ma, sa)
        keep(g + 1, mb, sb)
        return mb, sb, top_a

    zero = jnp.zeros((8, NT), F32)
    with jax.named_scope("pass1"):
        lax.fori_loop(0, TOTAL // 2, pass1, (zero, zero, logits_top(0, la)))

    scope = jax.named_scope("stats")
    scope.__enter__()
    stat_recv[chip] = stat[chip]

    def clear_de(i, carry):
        d_e[pl.ds(pl.multiple_of(i * COLS, COLS), COLS), :] = jnp.zeros((COLS, DIM), F32)
        e_t[:, pl.ds(pl.multiple_of(i * COLS, COLS), COLS)] = e_full[pl.ds(pl.multiple_of(i * COLS, COLS), COLS), :].T
        return carry

    def clear_dhn(i, carry):
        dhn_buf[i] = jnp.zeros((DIM, TOK), F32)
        return carry

    lax.fori_loop(0, NCHIP, clear_dhn, 0)
    for mask in MASKS:
        there = flip(chip, mask)
        pltpu.make_async_remote_copy(stat.at[there], stat_recv.at[there], sts.at[there], str_.at[there], **same_core(there)).wait_recv()
    stats = stat_recv[...]
    top = jnp.max(stats, axis=0)
    lse_own[...] = top + jnp.log(jnp.sum(jnp.exp2(stats - top[None]), axis=0)) * LOG2E

    def lse_copy(there, slot):
        return pltpu.make_async_remote_copy(lse_own, lse_all.at[slot], lss.at[there], lsr.at[slot], **same_core(there))

    for mask in MASKS:
        lse_copy(flip(chip, mask), chip).start()
    lse_all[chip] = lse_own[...]
    lax.fori_loop(0, V_CHIP // COLS, clear_de, 0)
    for mask in MASKS:
        there = flip(chip, mask)
        lse_copy(there, there).wait_recv()

    scope.__exit__(None, None, None)

    iota = lax.broadcasted_iota(jnp.int32, (16, NT), 0)

    def soften(g, tile, out, acc):
        _, b, n0, t = where_is(g, True)
        c = coef[b, :, pl.ds(n0, NT)]
        shift = jnp.where(c > 0.0, lse_all[b, :, pl.ds(n0, NT)] - jnp.log(jnp.where(c > 0.0, c, 1.0)) * LOG2E, jnp.inf)
        where = lab[b, :, pl.ds(n0, NT)] - t * TV
        c = jnp.broadcast_to(c, (16, NT))
        shift = jnp.broadcast_to(shift, (16, NT))
        where = jnp.broadcast_to(where, (16, NT))
        for r in range(TV // 16):
            x = tile[16 * r : 16 * r + 16, :]
            w = jnp.where(iota + 16 * r == where, c, 0.0)
            out[16 * r : 16 * r + 16, :] = (jnp.exp2(x * LOG2E - shift) - w).astype(BF16)
            y = w * x
            acc = acc + (y[:8] + y[8:])
        return acc

    def products(g, d):
        k, b, n0, t = where_is(g, True)
        rows = pl.ds(pl.multiple_of(t * TV, TV), TV)
        d_e[rows, :] += jnp.dot(d[...], hn_all[b, pl.ds(n0, NT), :], preferred_element_type=F32)
        dhn_buf[k, :, pl.ds(n0, NT)] += jnp.dot(e_t[:, rows], d[...], preferred_element_type=F32)

    def dhn_copy(k, there, slot):
        return pltpu.make_async_remote_copy(dhn_buf.at[k], dhn_recv.at[slot], ds_.at[k], dr.at[slot], **same_core(there))

    logits(0, True, la)
    logits(1, True, lb)
    picked = soften(0, la, da, zero)

    def pass2(i, picked):
        g = 2 * i
        logits(g + 2, True, la)
        picked = soften(g + 1, lb, db, picked)
        products(g, da)
        logits(g + 3, True, lb)
        picked = soften(g + 2, la, da, picked)
        products(g + 1, db)

        @pl.when(lax.rem(g + 2, PER_BLOCK) == 0)
        def _():
            k, b, _, _ = where_is(g, True)
            dhn_copy(k, b, chip).start()

        return picked

    with jax.named_scope("pass2"):
        picked = lax.fori_loop(0, TOTAL // 2 - 1, pass2, picked)
    picked = soften(TOTAL - 1, lb, db, picked)
    products(TOTAL - 2, da)
    products(TOTAL - 1, db)

    def de_copy(rows):
        return pltpu.make_async_remote_copy(d_e.at[rows], de_o, xs, xr, device_id=(partner,), device_id_type=MESH)

    de_copy(theirs).start()
    own = jnp.sum(coef[chip] * lse_own[...] * LN2, axis=1, keepdims=True)
    picked = jnp.sum(jnp.sum(picked, axis=0, keepdims=True), axis=1, keepdims=True)
    loss_o[...] = jnp.broadcast_to(own - picked, loss_o.shape)
    with jax.named_scope("dhn_wait"):
        for mask in MASKS:
            there = flip(chip, mask)
            dhn_copy(7 - mask, there, there).wait_recv()
    dhn_recv[chip] = dhn_buf[7]
    total = dhn_recv[0]
    for j in range(1, NCHIP):
        total = total + dhn_recv[j]
    dhn_o[...] = total
    de_copy(theirs).wait()
    de_o[...] += d_e[mine, :]

    for mask in MASKS:
        there = flip(chip, mask)
        hn_copy(there, chip).wait_send()
        pltpu.make_async_remote_copy(stat.at[there], stat_recv.at[chip], sts.at[there], str_.at[chip], **same_core(there)).wait_send()
        lse_copy(there, chip).wait_send()
        dhn_copy(7 - mask, there, chip).wait_send()


def head(hn, table, lab, coef):
    dma = pltpu.SemaphoreType.DMA
    vm = pltpu.VMEM
    eight = [dma((NCHIP,)), dma((NCHIP,))]
    one = [dma(()), dma(())]
    return pl.pallas_call(
        head_kernel,
        name="head",
        out_shape=[jax.ShapeDtypeStruct((DIM, TOK), F32), jax.ShapeDtypeStruct((ROWS, DIM), F32), jax.ShapeDtypeStruct((1, 128), F32)],
        in_specs=[VMEM_SPEC] * 4,
        out_specs=[VMEM_SPEC] * 3,
        scratch_shapes=[
            vm((NCHIP, TOK, DIM), BF16), vm((V_CHIP, DIM), BF16), vm((DIM, V_CHIP), BF16), vm((V_CHIP, DIM), F32),
            vm((NCHIP, DIM, TOK), F32), vm((NCHIP, DIM, TOK), F32),
            vm((NCHIP, 1, TOK), F32), vm((NCHIP, 1, TOK), F32), vm((1, TOK), F32), vm((NCHIP, 1, TOK), F32),
            vm((TV, NT), F32), vm((TV, NT), F32), vm((TV, NT), BF16), vm((TV, NT), BF16),
        ]
        + eight + one + eight + eight + eight + one,
        compiler_params=params(4, 63),
    )(hn, table, lab, coef)


def rms_scale(rows_wide, norm_gain):
    inv_rms = lax.rsqrt(jnp.mean(rows_wide * rows_wide, axis=-1, keepdims=True) + NORM_EPS)
    return (rows_wide * inv_rms * norm_gain).astype(BF16), inv_rms


def rms_back(rows_wide, inv_rms, norm_gain, grad_out):
    scaled_grad = grad_out * norm_gain
    return inv_rms * (scaled_grad - rows_wide * (inv_rms * inv_rms) * jnp.mean(scaled_grad * rows_wide, axis=-1, keepdims=True))


def solution(mesh):
    def device_step(tok_ids, tok_labels, loss_mask, table, gain_mlp, gain_head, gate_shard, up_shard, down_shard):
        meta = jnp.stack([tok_ids, tok_labels, loss_mask])[:, None, :]
        gains = (gain_mlp[None], gain_head[None])
        ids_all, lab_rel, coef, pos, emb_rows, local, *acts, gate_full, up_full, down_full = start(meta, gate_shard, up_shard, down_shard, table, *gains)

        devices = jnp.arange(NDEV, dtype=jnp.int32)
        counts = jnp.sum(((ids_all // ROWS)[:, None, :] == devices[None, :, None]).astype(jnp.int32), axis=2)
        rounds = (jnp.max(counts) + CAP - 1) // CAP
        slots = jnp.arange(NDEV * CAP, dtype=jnp.int32)

        def places(ids_all, tok_ids):
            upper = jnp.triu(jnp.ones((TOK, TOK), BF16), 1)
            lids = ids_all - lax.axis_index("fsdp") * ROWS
            owned = (lids >= 0) & (lids < ROWS)
            key = jnp.where(owned, jnp.dot(owned.astype(BF16), upper, preferred_element_type=F32).astype(jnp.int32), -1)
            owner = tok_ids // ROWS
            is_owner = owner[None, :] == devices[:, None]
            my_rank = jnp.sum(jnp.where(is_owner, jnp.dot(is_owner.astype(BF16), upper, preferred_element_type=F32), 0.0), axis=0).astype(jnp.int32)

            def place(r):
                slot = my_rank - r * CAP
                return jnp.where((slot >= 0) & (slot < CAP), owner * CAP + slot, -1)

            return lids, key, place

        def more_rows(rows, acts, ids_all, tok_ids, table):
            lids, key, place = places(ids_all, tok_ids)

            def one(r, rows):
                got, _ = fetch_rows(key - r * CAP, lids, table)
                pick = (place(r)[:, None] == slots[None, :]).astype(BF16)
                return rows + jnp.dot(pick, got.reshape(NDEV * CAP, DIM), preferred_element_type=F32).astype(BF16)

            rows = lax.fori_loop(1, rounds, one, rows)
            return rows, tuple(forward_again(rows, *gains, gate_full, up_full, down_full))

        emb_rows, acts = lax.cond(rounds > 1, more_rows, lambda rows, acts, *_: (rows, acts), emb_rows, tuple(acts), ids_all, tok_ids, table)
        hid, h_norm = acts
        d_hnorm_t, head_grad, loss_part = head(h_norm, table, lab_rel, coef)
        where = local.reshape(1, NDEV * CAP).astype(jnp.int32)
        grad_table, out_gate, out_up, out_down, loss, grad_x = finish(
            pos, d_hnorm_t, emb_rows, hid, gate_full, up_full, down_full, *gains, where, head_grad, loss_part
        )

        def more_grads(acc, ids_all, tok_ids, grad_x):
            lids, key, place = places(ids_all, tok_ids)

            def one(r, acc):
                got = send_grads(place(r)[None], grad_x)
                hit = (key - r * CAP)[:, None, :] == jnp.arange(CAP, dtype=jnp.int32)[None, :, None]
                return add_rows(jnp.sum(jnp.where(hit, (lids + 1)[:, None, :], 0), axis=2), got, acc)

            return lax.fori_loop(1, rounds, one, acc)

        grad_table = lax.cond(rounds > 1, more_grads, lambda acc, *_: acc, grad_table, ids_all, tok_ids, grad_x)
        return loss[0, 0], grad_table, out_gate, out_up, out_down

    row_spec = P("fsdp", None)
    tok_spec = P("fsdp")
    return jax.shard_map(device_step, mesh=mesh, in_specs=(tok_spec, tok_spec, tok_spec, row_spec, P(), P(), row_spec, row_spec, row_spec), out_specs=(P(), row_spec, row_spec, row_spec, row_spec), check_vma=False)
```

```python
import functools

import jax
import jax.numpy as jnp
from jax import lax
from jax.experimental import pallas as pl
from jax.experimental.pallas import tpu as pltpu
from jax.sharding import PartitionSpec as P

NORM_EPS = 1e-6
ROW_CONTRACT = (((1,), (1,)), ((), ()))
TOK_CONTRACT = (((0,), (0,)), ((), ()))
MESH = pl.DeviceIdType.MESH
F32 = jnp.float32
BF16 = jnp.bfloat16
LOG2E = 1.4426950408889634
LN2 = 0.6931471805599453

NDEV = 16
NCHIP = 8
ROWS = 3584
TOK = 1024
DIM = 256
FF = 1536
CAP = 96
TV = 1024
NT = 512
V_CHIP = 2 * ROWS
NTILE = V_CHIP // TV
NCHUNK = TOK // NT
PER_BLOCK = NTILE * NCHUNK
TOTAL = NCHIP * PER_BLOCK


def flip(chip, mask):
    out = 0
    for bit in (1, 2, 4):
        a, m = lax.rem(lax.div(chip, bit), 2), lax.rem(lax.div(mask, bit), 2)
        out = out + (a + m - 2 * a * m) * bit
    return out


AXES = ((2, 4, 1), (4, 1, 2), (1, 2, 4))
OTHERS = range(1, NDEV)
MASKS = range(1, NCHIP)
COLS = 256
THREE = range(3)
EACH = (3, NCHIP)


def whereabouts():
    me = lax.axis_index("fsdp")
    chip, core = lax.div(me, 2), lax.rem(me, 2)
    return me, chip, core, me + 1 - core - core


def side(chip, bit):
    return lax.rem(lax.div(chip, bit), 2)


def turn(chip, bits):
    out = chip
    for bit in bits:
        out = out + bit * (1 - 2 * side(chip, bit))
    return out


def barrier_greet(me):
    bar = pltpu.get_barrier_semaphore()
    for k in OTHERS:
        pl.semaphore_signal(bar, inc=1, device_id=(lax.rem(me + k, NDEV),), device_id_type=MESH)


def barrier_wait():
    pl.semaphore_wait(pltpu.get_barrier_semaphore(), NDEV - 1)


def barrier_all(me):
    barrier_greet(me)
    barrier_wait()


def params(cid, mib):
    return pltpu.CompilerParams(collective_id=cid, has_side_effects=True, vmem_limit_bytes=mib * 2**20)


VMEM_SPEC = pl.BlockSpec(memory_space=pltpu.VMEM)


def pack_rows(ids_key, ids_local, table, send, local):
    slot_iota = lax.broadcasted_iota(jnp.int32, (CAP, TOK), 0)
    for d in range(NDEV):
        hit = ids_key[d : d + 1, :] == slot_iota
        local[d] = jnp.sum(jnp.where(hit, ids_local[d : d + 1, :] + 1, 0).astype(F32), axis=1, keepdims=True)

    group = 4
    row_iota = lax.broadcasted_iota(jnp.int32, (group * CAP, COLS), 1)

    def pack(g, carry):
        col = jnp.concatenate([local[g * group + j] for j in range(group)], axis=0).astype(jnp.int32)
        acc = jnp.zeros((group * CAP, DIM), F32)
        for v in range(ROWS // COLS):
            pick = jnp.where(row_iota + (v * COLS + 1) == col, 1.0, 0.0).astype(BF16)
            acc = acc + jnp.dot(pick, table[v * COLS : (v + 1) * COLS, :], preferred_element_type=F32)
        rows = acc.astype(BF16)
        for j in range(group):
            send[g * group + j] = rows[j * CAP : (j + 1) * CAP]
        return carry

    lax.fori_loop(0, NDEV // group, pack, 0)


STEP = 256


def forward_again(x, gain_mlp, gain_head, gate, up, down):
    shape = jax.ShapeDtypeStruct
    return pl.pallas_call(
        mlp_rows,
        name="forward_again",
        out_shape=[shape((TOK, DIM), BF16)] * 2,
        in_specs=[VMEM_SPEC] * 6,
        out_specs=[VMEM_SPEC] * 2,
        compiler_params=pltpu.CompilerParams(vmem_limit_bytes=48 * 2**20),
    )(x, gain_mlp, gain_head, gate, up, down)


def wide_weights(gate, up, down):
    return gate[...].reshape(DIM, FF), up[...].reshape(DIM, FF), down[...].reshape(FF, DIM)


def swiglu(a, w_gate, w_up):
    p = jnp.dot(a, w_gate, preferred_element_type=F32).astype(BF16).astype(F32)
    q = jnp.dot(a, w_up, preferred_element_type=F32).astype(BF16).astype(F32)
    sig = jax.nn.sigmoid(p)
    return p, q, sig, (p * sig * q).astype(BF16)


def mlp_rows(x, gain_mlp, gain_head, gate, up, down, h_o, hn_o):
    def some(i, carry):
        rows = pl.ds(pl.multiple_of(i * STEP, STEP), STEP)
        w_gate, w_up, w_down = wide_weights(gate, up, down)
        wide = x[rows, :].astype(F32)
        a = rms_scale(wide, gain_mlp[...])[0]
        u = swiglu(a, w_gate, w_up)[3]
        h = (wide + jnp.dot(u, w_down, preferred_element_type=F32)).astype(BF16)
        h_o[rows, :] = h
        hn_o[rows, :] = rms_scale(h.astype(F32), gain_head[...])[0]
        return carry

    lax.fori_loop(0, TOK // STEP, some, 0)


def make_upper(upper):
    for r in range(TOK // 128):
        rows = lax.broadcasted_iota(jnp.int32, (128, TOK), 0) + 128 * r
        cols = lax.broadcasted_iota(jnp.int32, (128, TOK), 1)
        upper[128 * r : 128 * r + 128, :] = jnp.where(rows < cols, 1.0, 0.0).astype(BF16)


def start_kernel(meta, gate, up, down, table, gain_mlp, gain_head, ids_o, lab_o, coef_o, pos_o, full_o, x_o, local, h_o, hn_o, gate_o, up_o, down_o,
                 meta_all, key, lid, upper, send, recv, total, ms, mr, ws, wr, fs, fr, ss, rs):
    me, chip, core, partner = whereabouts()
    barrier_greet(me)
    make_upper(upper)
    barrier_wait()
    sends = []
    for k in OTHERS:
        cp = pltpu.make_async_remote_copy(meta, meta_all.at[me], ms.at[k], mr.at[me], device_id=(lax.rem(me + k, NDEV),), device_id_type=MESH)
        cp.start()
        sends.append(cp)
    srcs, outs = (gate, up, down), (gate_o, up_o, down_o)

    def forward(i, src, slot, there):
        return pltpu.make_async_remote_copy(src, outs[i].at[slot], fs.at[i, there], fr.at[i, there], device_id=(partner,), device_id_type=MESH)

    def hop(i, stage, go):
        axes = AXES[i]
        turns = [()]
        for bit in axes[:stage]:
            turns = turns + [bits + (bit,) for bits in turns]
        across = 2 * turn(chip, axes[stage : stage + 1]) + core
        for n, bits in enumerate(turns):
            slot = len(turns) - 1 + n
            there = turn(chip, bits if go else bits + axes[stage : stage + 1])
            block = outs[i].at[2 * there + core]
            cp = pltpu.make_async_remote_copy(srcs[i] if go and not bits else block, block, ws.at[i, slot], wr.at[i, slot], device_id=(across,), device_id_type=MESH)
            if not go:
                cp.wait_recv()
                cp = forward(i, block, 2 * there + core, there)
            cp.start()
            sends.append(cp)

    for i in THREE:
        hop(i, 0, True)
    for i in THREE:
        cp = forward(i, srcs[i], me, chip)
        cp.start()
        sends.append(cp)
        outs[i][me] = srcs[i][...]
    meta_all[me] = meta[...]
    for k in OTHERS:
        other = lax.rem(me + k, NDEV)
        pltpu.make_async_remote_copy(meta, meta_all.at[other], ms.at[k], mr.at[other], device_id=(other,), device_id_type=MESH).wait_recv()

    for i in THREE:
        hop(i, 0, False)
        hop(i, 1, True)

    for d in range(NDEV):
        ids_o[d : d + 1, :] = meta_all[d, 0]
    lids = ids_o[...] - me * ROWS
    owned = (lids >= 0) & (lids < ROWS)
    rank = jnp.dot(jnp.where(owned, 1.0, 0.0).astype(BF16), upper[...], preferred_element_type=F32).astype(jnp.int32)
    key[...] = jnp.where(owned, rank, -1)
    lid[...] = lids
    with jax.named_scope("s_pack"):
        pack_rows(key, lid, table, send, local)
    send_blocks(me, send, recv, ss, rs)
    for i in THREE:
        hop(i, 1, False)
        hop(i, 2, True)
    recv[me] = send[me]

    count = meta_all[0, 2]
    for d in range(1, NDEV):
        count = count + meta_all[d, 2]
    n_all = jnp.sum(count.astype(F32), axis=1, keepdims=True)
    for j in range(NCHIP):
        lab_o[j] = meta_all[2 * j + core, 1] - chip * V_CHIP
        coef_o[j] = meta_all[2 * j + core, 2].astype(F32) / n_all

    full = jnp.zeros((NDEV, 1), F32)
    for d in range(NDEV):
        far = ids_o[...] - d * ROWS
        full = jnp.maximum(full, jnp.sum(jnp.where((far >= 0) & (far < ROWS), 1.0, 0.0), axis=1, keepdims=True))
    full_o[...] = jnp.broadcast_to(jnp.max(full, axis=0, keepdims=True), full_o.shape).astype(jnp.int32)

    first = lax.broadcasted_iota(jnp.int32, (NDEV, TOK), 0) * ROWS
    mine = meta[0]
    is_owner = (mine >= first) & (mine < first + ROWS)
    rank = jnp.dot(jnp.where(is_owner, 1.0, 0.0).astype(BF16), upper[...], preferred_element_type=F32).astype(jnp.int32)
    slot = jnp.where(is_owner & (rank < CAP), lax.broadcasted_iota(jnp.int32, (NDEV, TOK), 0) * CAP + rank, -1)
    pos_o[...] = jnp.max(slot, axis=0, keepdims=True)

    for i in THREE:
        hop(i, 2, False)
    with jax.named_scope("s_wait"):
        wait_blocks(me, send, recv, ss, rs)
    group = 4
    for g in range(NDEV // group):
        iota = lax.broadcasted_iota(jnp.int32, (group * CAP, TOK), 0) + g * group * CAP
        pick = jnp.where(iota == pos_o[...], 1.0, 0.0).astype(BF16)
        rows = jnp.concatenate([recv[g * group + j] for j in range(group)], axis=0)
        part = lax.dot_general(pick, rows, TOK_CONTRACT, preferred_element_type=F32)
        total[...] = part if g == 0 else total[...] + part
    x_o[...] = total[...].astype(BF16)
    for mask in range(NCHIP):
        there = flip(chip, mask)
        for i in THREE:
            forward(i, srcs[i], 2 * there + 1 - core, there).wait_recv()
    with jax.named_scope("s_mlp"):
        mlp_rows(x_o, gain_mlp, gain_head, gate_o, up_o, down_o, h_o, hn_o)
    for cp in sends:
        cp.wait_send()


def start(meta, gate, up, down, table, gain_mlp, gain_head):
    dma = pltpu.SemaphoreType.DMA
    vm = pltpu.VMEM
    shape = jax.ShapeDtypeStruct
    return pl.pallas_call(
        start_kernel,
        name="start",
        out_shape=[
            shape((NDEV, TOK), jnp.int32), shape((NCHIP, 1, TOK), jnp.int32), shape((NCHIP, 1, TOK), F32), shape((1, TOK), jnp.int32), shape((1, 128), jnp.int32),
            shape((TOK, DIM), BF16), shape((NDEV, CAP, 1), F32),
        ]
        + [shape((TOK, DIM), BF16)] * 2
        + [shape((NDEV,) + a.shape, a.dtype) for a in (gate, up, down)],
        in_specs=[VMEM_SPEC] * 7,
        out_specs=[VMEM_SPEC] * 12,
        scratch_shapes=[
            vm((NDEV, 3, 1, TOK), jnp.int32), vm((NDEV, TOK), jnp.int32), vm((NDEV, TOK), jnp.int32), vm((TOK, TOK), BF16),
            vm((NDEV, CAP, DIM), BF16), vm((NDEV, CAP, DIM), BF16), vm((TOK, DIM), F32),
            dma((NDEV,)), dma((NDEV,)), dma(EACH), dma(EACH), dma(EACH), dma(EACH), dma((NDEV,)), dma((NDEV,)),
        ],
        compiler_params=params(0, 60),
    )(meta, gate, up, down, table, gain_mlp, gain_head)


def send_blocks(me, send, recv, ss, rs):
    def start(k, carry):
        other = lax.rem(me + k, NDEV)
        pltpu.make_async_remote_copy(send.at[other], recv.at[me], ss.at[other], rs.at[me], device_id=(other,), device_id_type=MESH).start()
        return carry

    lax.fori_loop(1, NDEV, start, 0)


def wait_blocks(me, send, recv, ss, rs):
    def wait(k, carry):
        other = lax.rem(me + k, NDEV)
        pltpu.make_async_remote_copy(send.at[other], recv.at[other], ss.at[other], rs.at[other], device_id=(other,), device_id_type=MESH).wait()
        return carry

    lax.fori_loop(1, NDEV, wait, 0)


def rows_kernel(keys, lids, table, recv, local, send, ss, rs):
    me = lax.axis_index("fsdp")
    barrier_all(me)
    pack_rows(keys, lids, table, send, local)
    send_blocks(me, send, recv, ss, rs)
    recv[me] = send[me]
    wait_blocks(me, send, recv, ss, rs)


def fetch_rows(keys, lids, table):
    dma = pltpu.SemaphoreType.DMA
    return pl.pallas_call(
        rows_kernel,
        name="fetch_rows",
        out_shape=[jax.ShapeDtypeStruct((NDEV, CAP, DIM), BF16), jax.ShapeDtypeStruct((NDEV, CAP, 1), F32)],
        in_specs=[VMEM_SPEC] * 3,
        out_specs=[VMEM_SPEC] * 2,
        scratch_shapes=[pltpu.VMEM((NDEV, CAP, DIM), BF16), dma((NDEV,)), dma((NDEV,))],
        compiler_params=params(1, 40),
    )(keys, lids, table)


def split3(wide):
    hi = wide.astype(BF16)
    rest = wide - hi.astype(F32)
    mid = rest.astype(BF16)
    return hi, mid, (rest - mid.astype(F32)).astype(BF16)


def put_parts(parts, rows, wide):
    for n, part in enumerate(split3(wide)):
        parts[rows, n * DIM : (n + 1) * DIM] = part


def add_parts(sums):
    return (sums[:, :DIM] + sums[:, DIM : 2 * DIM]) + sums[:, 2 * DIM :]


def pack_grads(me, pos, dx, send, recv, parts, ss, rs):
    put_parts(parts, slice(None), dx[...])
    slot_iota = lax.broadcasted_iota(jnp.int32, (CAP, TOK), 0)

    def pack(k, carry):
        other = lax.rem(me + k, NDEV)
        pick = jnp.where(pos[0:1, :] - other * CAP == slot_iota, 1.0, 0.0).astype(BF16)
        rows = jnp.dot(pick, parts[...], preferred_element_type=F32)
        send[other] = add_parts(rows)

        @pl.when(k < NDEV)
        def _():
            pltpu.make_async_remote_copy(send.at[other], recv.at[me], ss.at[other], rs.at[me], device_id=(other,), device_id_type=MESH).start()

        return carry

    lax.fori_loop(1, NDEV + 1, pack, 0)


def grads_kernel(pos, dx, recv, send, parts, ss, rs):
    me = lax.axis_index("fsdp")
    barrier_all(me)
    pack_grads(me, pos, dx, send, recv, parts, ss, rs)
    recv[me] = send[me]
    wait_blocks(me, send, recv, ss, rs)


def send_grads(pos, dx):
    dma = pltpu.SemaphoreType.DMA
    return pl.pallas_call(
        grads_kernel,
        name="send_grads",
        out_shape=jax.ShapeDtypeStruct((NDEV, CAP, DIM), F32),
        in_specs=[VMEM_SPEC] * 2,
        out_specs=VMEM_SPEC,
        scratch_shapes=[pltpu.VMEM((NDEV, CAP, DIM), F32), pltpu.VMEM((TOK, 3 * DIM), BF16), dma((NDEV,)), dma((NDEV,))],
        compiler_params=params(2, 40),
    )(pos, dx)


def add_kernel(local, rows, base, out, parts):
    @pl.when(pl.program_id(0) == 0)
    def _():
        put_parts(parts, slice(None), rows[...])

    first = pl.program_id(0) * COLS + 1
    iota = lax.broadcasted_iota(jnp.int32, (COLS, NDEV * CAP), 0) + first
    pick = jnp.where(iota == local[...], 1.0, 0.0).astype(BF16)
    sums = jnp.dot(pick, parts[...], preferred_element_type=F32)
    out[...] = base[...] + add_parts(sums)


def add_rows(local, rows, base):
    n = NDEV * CAP
    return pl.pallas_call(
        add_kernel,
        name="add_rows",
        grid=(ROWS // COLS,),
        out_shape=jax.ShapeDtypeStruct((ROWS, DIM), F32),
        in_specs=[pl.BlockSpec((1, n), lambda i: (0, 0)), pl.BlockSpec((n, DIM), lambda i: (0, 0)), pl.BlockSpec((COLS, DIM), lambda i: (i, 0))],
        out_specs=pl.BlockSpec((COLS, DIM), lambda i: (i, 0)),
        scratch_shapes=[pltpu.VMEM((n, 3 * DIM), BF16)],
        compiler_params=pltpu.CompilerParams(vmem_limit_bytes=40 * 2**20),
    )(local.reshape(1, n).astype(jnp.int32), rows.reshape(n, DIM), base)


def weight_grad(left, right, out):
    grad = lax.dot_general(left[...], right[...], TOK_CONTRACT, preferred_element_type=F32)
    rows = out.shape[2]
    for j in range(NDEV):
        out[j // 2, j % 2] = grad[j * rows : (j + 1) * rows]


def finish_kernel(pos, dhn, x, h, w_gate, w_up, w_down, gain_mlp, gain_head, where, base, loss, table_o, gate_o, up_o, down_o, loss_o, dx,
                  gate, up, down, dhid, dhid_b, a_all, u_all, dgate, dup, send, recv, parts, rparts, pg, pu, pd, sg, su, sd, rg, ru, rd, ls, xs, xr, ps, pr, ss, rs, lss, lrs):
    me, chip, core, partner = whereabouts()
    barrier_greet(me)
    srcs, pairs, sums, recvs, outs = (gate, up, down), (pg, pu, pd), (sg, su, sd), (rg, ru, rd), (gate_o, up_o, down_o)
    sends = []

    def pair(i):
        return pltpu.make_async_remote_copy(srcs[i].at[:, 1 - core], pairs[i], ps.at[i], pr.at[i], device_id=(partner,), device_id_type=MESH)

    def back(n, carry):
        rows = pl.ds(pl.multiple_of(n * STEP, STEP), STEP)
        wide = h[rows, :].astype(F32)
        inv = rms_scale(wide, gain_head[...])[1]
        grad = rms_back(wide, inv, gain_head[...], dhn[:, rows].T)
        dhid[rows, :] = grad
        grad = grad.astype(BF16)
        dhid_b[rows, :] = grad
        a = rms_scale(x[rows, :].astype(F32), gain_mlp[...])[0]
        a_all[rows, :] = a
        g_full, u_full, d_full = wide_weights(w_gate, w_up, w_down)
        p, q, sig, act = swiglu(a, g_full, u_full)
        u_all[rows, :] = act
        dact = lax.dot_general(grad, d_full, ROW_CONTRACT, preferred_element_type=F32)
        dup[rows, :] = (dact * p * sig).astype(BF16)
        dgate[rows, :] = (dact * q * sig * (1.0 + p * (1.0 - sig))).astype(BF16)
        return carry

    with jax.named_scope("f_back"):
        lax.fori_loop(0, TOK // STEP, back, 0)
    def hop(i, stage, go):
        b1, b2, b3 = AXES[i]
        base_1, base_2 = side(chip, b1) * b1, side(chip, b2) * b2
        if stage == 0:
            bit, blocks = b1, [(n, n // 2 * b2 + n % 2 * b3) for n in range(4)]
            lead = 0
        elif stage == 1:
            bit, blocks = b2, [(4 + n, n * b3) for n in range(2)]
            lead = base_1
        else:
            bit, blocks = b3, [(6, 0)]
            lead = base_1 + base_2
        across = 2 * turn(chip, (bit,)) + core
        for slot, rest in blocks:
            out_block = lead + (1 - side(chip, bit)) * bit + rest
            in_block = lead + side(chip, bit) * bit + rest
            cp = pltpu.make_async_remote_copy(sums[i].at[out_block], recvs[i].at[slot], ss.at[i, slot], rs.at[i, slot], device_id=(across,), device_id_type=MESH)
            if go:
                cp.start()
                sends.append(cp)
            elif stage < 2:
                cp.wait_recv()
                sums[i][in_block] = sums[i][in_block] + recvs[i][slot]
            else:
                cp.wait_recv()
                outs[i][...] = sums[i][chip] + recvs[i][slot]

    def merge(i):
        pair(i).wait()
        sums[i][...] = srcs[i][:, core] + pairs[i][...]
        hop(i, 0, True)

    def to_rows(n, carry):
        rows = pl.ds(pl.multiple_of(n * STEP, STEP), STEP)
        da = lax.dot_general(dgate[rows, :], w_gate[...].reshape(DIM, FF), ROW_CONTRACT, preferred_element_type=F32)
        da = da + lax.dot_general(dup[rows, :], w_up[...].reshape(DIM, FF), ROW_CONTRACT, preferred_element_type=F32)
        wide = x[rows, :].astype(F32)
        inv = rms_scale(wide, gain_mlp[...])[1]
        dx[rows, :] = dhid[rows, :] + rms_back(wide, inv, gain_mlp[...], da)
        return carry

    lax.fori_loop(0, TOK // STEP, to_rows, 0)
    with jax.named_scope("f_pack"):
        barrier_wait()
        pack_grads(me, pos, dx, send, recv, parts, xs, xr)
    weight_grad(u_all, dhid_b, down)
    pair(2).start()
    weight_grad(a_all, dgate, gate)
    pair(0).start()
    weight_grad(a_all, dup, up)
    pair(1).start()
    for i in (2, 0, 1):
        merge(i)
    for k in OTHERS:
        cp = pltpu.make_async_remote_copy(loss, ls.at[me], lss.at[k], lrs.at[me], device_id=(lax.rem(me + k, NDEV),), device_id_type=MESH)
        cp.start()
        sends.append(cp)
    ls[me] = loss[...]
    recv[me] = send[me]
    with jax.named_scope("f_wait"):
        wait_blocks(me, send, recv, xs, xr)
    for d in range(NDEV):
        put_parts(rparts, slice(d * CAP, (d + 1) * CAP), recv[d])

    def add(v, carry):
        rows = pl.ds(pl.multiple_of(v * NT, NT), NT)
        iota = lax.broadcasted_iota(jnp.int32, (NT, NDEV * CAP), 0) + (v * NT + 1)
        pick = jnp.where(iota == where[...], 1.0, 0.0).astype(BF16)
        got = jnp.dot(pick, rparts[...], preferred_element_type=F32)
        table_o[rows, :] = base[rows, :] + add_parts(got)
        return carry

    with jax.named_scope("f_add"):
        lax.fori_loop(0, 2, add, 0)
        for stage in (0, 1):
            for i in THREE:
                hop(i, stage, False)
                hop(i, stage + 1, True)
            lax.fori_loop(2 * stage + 2, 2 * stage + 4, add, 0)
        lax.fori_loop(6, ROWS // NT, add, 0)
    for i in THREE:
        hop(i, 2, False)
    for k in OTHERS:
        other = lax.rem(me + k, NDEV)
        pltpu.make_async_remote_copy(loss, ls.at[other], lss.at[k], lrs.at[other], device_id=(other,), device_id_type=MESH).wait_recv()
    loss_o[...] = jnp.sum(ls[...], axis=0)
    for cp in sends:
        cp.wait_send()


def finish(pos, dhn, x, h, gate, up, down, gain_mlp, gain_head, where, base, loss):
    dma = pltpu.SemaphoreType.DMA
    vm = pltpu.VMEM
    big = [jax.ShapeDtypeStruct((NCHIP, 2) + a.shape[1:], F32) for a in (gate, up, down)]
    buffers = [vm((NCHIP,) + a.shape[2:], F32) for a in big]
    back = [vm(a.shape, F32) for a in big] + [vm((TOK, DIM), F32), vm((TOK, DIM), BF16), vm((TOK, DIM), BF16), vm((TOK, FF), BF16), vm((TOK, FF), BF16), vm((TOK, FF), BF16)]
    return pl.pallas_call(
        finish_kernel,
        name="finish",
        out_shape=[jax.ShapeDtypeStruct((ROWS, DIM), F32)] + [jax.ShapeDtypeStruct(a.shape[2:], F32) for a in big] + [jax.ShapeDtypeStruct(loss.shape, F32), jax.ShapeDtypeStruct((TOK, DIM), F32)],
        in_specs=[VMEM_SPEC] * 12,
        out_specs=[VMEM_SPEC] * 6,
        scratch_shapes=back + [vm((NDEV, CAP, DIM), F32), vm((NDEV, CAP, DIM), F32), vm((TOK, 3 * DIM), BF16), vm((NDEV * CAP, 3 * DIM), BF16)]
        + buffers * 3
        + [vm((NDEV,) + loss.shape, F32), dma((NDEV,)), dma((NDEV,)), dma((3,)), dma((3,)), dma(EACH), dma(EACH), dma((NDEV,)), dma((NDEV,))],
        compiler_params=params(3, 63),
    )(pos, dhn, x, h, gate, up, down, gain_mlp, gain_head, where, base, loss)


def head_kernel(hn, e_own, lab, coef, dhn_o, de_o, loss_o, hn_all, e_full, e_t, d_e, dhn_buf, dhn_recv, stat, stat_all, lse_all, la, lb, da, db,
                hs, hr, es, er, sts, str_, ds_, dr, xs, xr):
    me, chip, core, partner = whereabouts()
    bar = pltpu.get_barrier_semaphore()
    pl.semaphore_signal(bar, inc=1, device_id=(partner,), device_id_type=MESH)
    for mask in MASKS:
        pl.semaphore_signal(bar, inc=1, device_id=(2 * flip(chip, mask) + core,), device_id_type=MESH)
    pl.semaphore_wait(bar, NCHIP)

    def same_core(there):
        return dict(device_id=(2 * there + core,), device_id_type=MESH)

    mine = pl.ds(pl.multiple_of(core * ROWS, ROWS), ROWS)
    theirs = pl.ds(pl.multiple_of((1 - core) * ROWS, ROWS), ROWS)
    e_copy = pltpu.make_async_remote_copy(e_own, e_full.at[mine], es, er, device_id=(partner,), device_id_type=MESH)
    e_copy.start()

    def hn_copy(there, slot):
        return pltpu.make_async_remote_copy(hn, hn_all.at[slot], hs.at[there], hr.at[slot], **same_core(there))

    for mask in MASKS:
        hn_copy(flip(chip, mask), chip).start()
    e_full[mine, :] = e_own[...]
    hn_all[chip] = hn[...]
    pltpu.make_async_remote_copy(e_own, e_full.at[theirs], es, er, device_id=(partner,), device_id_type=MESH).wait()

    def where_is(g, last):
        k = lax.div(g, PER_BLOCK)
        rest = lax.rem(g, PER_BLOCK)
        n, t = lax.div(rest, NTILE), lax.rem(rest, NTILE)
        return k, flip(chip, 7 - k if last else k), pl.multiple_of(n * NT, NT), t

    def logits(g, last, out):
        _, b, n0, t = where_is(g, last)
        out[...] = lax.dot_general(e_full[pl.ds(pl.multiple_of(t * TV, TV), TV), :], hn_all[b, pl.ds(n0, NT), :], ROW_CONTRACT, preferred_element_type=F32)


    def logits_top(g, out):
        _, b, n0, t = where_is(g, False)
        tile = lax.dot_general(e_full[pl.ds(pl.multiple_of(t * TV, TV), TV), :], hn_all[b, pl.ds(n0, NT), :], ROW_CONTRACT, preferred_element_type=F32)
        out[...] = tile
        return jnp.max(tile.reshape(TV // 8, 8, NT), axis=0)

    def update(tile, tile_top, first, m, s):
        m = jnp.where(first, -jnp.inf, m)
        top = jnp.maximum(m, tile_top * LOG2E)
        sums = [jnp.where(first, 0.0, s) * jnp.exp2(m - top)] + [None] * 3
        for r in range(TV // 8):
            e = jnp.exp2(tile[8 * r : 8 * r + 8, :] * LOG2E - top)
            sums[r % 4] = e if sums[r % 4] is None else sums[r % 4] + e
        return top, (sums[0] + sums[1]) + (sums[2] + sums[3])

    def stat_copy(mask, b, slot):
        return pltpu.make_async_remote_copy(stat.at[b], stat_all.at[slot, b], sts.at[mask, b], str_.at[slot, b], **same_core(flip(chip, mask)))

    def keep(g, m, s):
        _, b, n0, t = where_is(g, False)

        @pl.when(t == NTILE - 1)
        def _():
            top = jnp.max(m, axis=0, keepdims=True)
            tot = jnp.sum(s * jnp.exp2(m - top), axis=0, keepdims=True)
            stat[b, :, pl.ds(n0, NT)] = top + jnp.log(tot) * LOG2E

        @pl.when(lax.rem(g + 1, PER_BLOCK) == 0)
        def _():
            for mask in MASKS:
                stat_copy(mask, b, chip).start()

    def pass1(i, carry):
        m, s, top_a = carry
        g = 2 * i
        nxt = jnp.minimum(g + 2, TOTAL - 2)

        @pl.when((lax.rem(g + 2, PER_BLOCK) == 0) & (g + 2 < TOTAL))
        def _():
            _, bn, _, _ = where_is(nxt, False)
            hn_copy(bn, bn).wait_recv()

        top_b = logits_top(g + 1, lb)
        ma, sa = update(la, top_a, where_is(g, False)[3] == 0, m, s)
        top_a = logits_top(nxt, la)
        mb, sb = update(lb, top_b, where_is(g + 1, False)[3] == 0, ma, sa)
        keep(g, ma, sa)
        keep(g + 1, mb, sb)
        return mb, sb, top_a

    zero = jnp.zeros((8, NT), F32)
    with jax.named_scope("pass1"):
        lax.fori_loop(0, TOTAL // 2, pass1, (zero, zero, logits_top(0, la)))

    scope = jax.named_scope("stats")
    scope.__enter__()
    stat_all[chip] = stat[...]

    def clear_de(i, carry):
        d_e[pl.ds(pl.multiple_of(i * COLS, COLS), COLS), :] = jnp.zeros((COLS, DIM), F32)
        e_t[:, pl.ds(pl.multiple_of(i * COLS, COLS), COLS)] = e_full[pl.ds(pl.multiple_of(i * COLS, COLS), COLS), :].T
        return carry

    def clear_dhn(i, carry):
        dhn_buf[i] = jnp.zeros((DIM, TOK), F32)
        return carry

    lax.fori_loop(0, NCHIP, clear_dhn, 0)
    lax.fori_loop(0, V_CHIP // COLS, clear_de, 0)

    def stat_wait(n, carry):
        mask = lax.div(n, NCHIP)
        stat_copy(mask, lax.rem(n, NCHIP), flip(chip, mask)).wait_recv()
        return carry

    lax.fori_loop(NCHIP, NCHIP * NCHIP, stat_wait, 0)
    stats = [stat_all[j] for j in range(NCHIP)]
    top = functools.reduce(jnp.maximum, stats)
    lse_all[...] = top + jnp.log(sum(jnp.exp2(one - top) for one in stats)) * LOG2E
    scope.__exit__(None, None, None)

    iota = lax.broadcasted_iota(jnp.int32, (16, NT), 0)

    def soften(g, tile, out, acc):
        _, b, n0, t = where_is(g, True)
        c = coef[b, :, pl.ds(n0, NT)]
        shift = jnp.where(c > 0.0, lse_all[b, :, pl.ds(n0, NT)] - jnp.log(jnp.where(c > 0.0, c, 1.0)) * LOG2E, jnp.inf)
        where = lab[b, :, pl.ds(n0, NT)] - t * TV
        c = jnp.broadcast_to(c, (16, NT))
        shift = jnp.broadcast_to(shift, (16, NT))
        where = jnp.broadcast_to(where, (16, NT))
        for r in range(TV // 16):
            x = tile[16 * r : 16 * r + 16, :]
            w = jnp.where(iota + 16 * r == where, c, 0.0)
            out[16 * r : 16 * r + 16, :] = (jnp.exp2(x * LOG2E - shift) - w).astype(BF16)
            y = w * x
            acc = acc + (y[:8] + y[8:])
        return acc

    def products(g, d):
        k, b, n0, t = where_is(g, True)
        rows = pl.ds(pl.multiple_of(t * TV, TV), TV)
        dhn_buf[k, :, pl.ds(n0, NT)] += jnp.dot(e_t[:, rows], d[...], preferred_element_type=F32)
        d_e[rows, :] += jnp.dot(d[...], hn_all[b, pl.ds(n0, NT), :], preferred_element_type=F32)

    def dhn_copy(k, there, slot):
        return pltpu.make_async_remote_copy(dhn_buf.at[k], dhn_recv.at[slot], ds_.at[k], dr.at[slot], **same_core(there))

    logits(0, True, la)
    logits(1, True, lb)
    picked = soften(0, la, da, zero)

    def pass2(i, picked):
        g = 2 * i
        logits(g + 2, True, la)
        picked = soften(g + 1, lb, db, picked)
        products(g, da)
        logits(g + 3, True, lb)
        picked = soften(g + 2, la, da, picked)
        products(g + 1, db)

        @pl.when(lax.rem(g + 2, PER_BLOCK) == 0)
        def _():
            k, b, _, _ = where_is(g, True)
            dhn_copy(k, b, chip).start()

        return picked

    with jax.named_scope("pass2"):
        picked = lax.fori_loop(0, TOTAL // 2 - 1, pass2, picked)
    picked = soften(TOTAL - 1, lb, db, picked)
    products(TOTAL - 2, da)
    products(TOTAL - 1, db)

    def de_copy(rows):
        return pltpu.make_async_remote_copy(d_e.at[rows], de_o, xs, xr, device_id=(partner,), device_id_type=MESH)

    de_copy(theirs).start()
    own = jnp.sum(coef[chip] * lse_all[chip] * LN2, axis=1, keepdims=True)
    picked = jnp.sum(jnp.sum(picked, axis=0, keepdims=True), axis=1, keepdims=True)
    loss_o[...] = jnp.broadcast_to(own - picked, loss_o.shape)
    with jax.named_scope("dhn_wait"):
        for mask in MASKS:
            there = flip(chip, mask)
            dhn_copy(7 - mask, there, there).wait_recv()
    dhn_recv[chip] = dhn_buf[7]
    total = dhn_recv[0]
    for j in range(1, NCHIP):
        total = total + dhn_recv[j]
    dhn_o[...] = total
    de_copy(theirs).wait()
    de_o[...] += d_e[mine, :]

    for mask in MASKS:
        there = flip(chip, mask)
        hn_copy(there, chip).wait_send()
        for b in range(NCHIP):
            stat_copy(mask, b, chip).wait_send()
        dhn_copy(7 - mask, there, chip).wait_send()


def head(hn, table, lab, coef):
    dma = pltpu.SemaphoreType.DMA
    vm = pltpu.VMEM
    eight = [dma((NCHIP,)), dma((NCHIP,))]
    one = [dma(()), dma(())]
    return pl.pallas_call(
        head_kernel,
        name="head",
        out_shape=[jax.ShapeDtypeStruct((DIM, TOK), F32), jax.ShapeDtypeStruct((ROWS, DIM), F32), jax.ShapeDtypeStruct((1, 128), F32)],
        in_specs=[VMEM_SPEC] * 4,
        out_specs=[VMEM_SPEC] * 3,
        scratch_shapes=[
            vm((NCHIP, TOK, DIM), BF16), vm((V_CHIP, DIM), BF16), vm((DIM, V_CHIP), BF16), vm((V_CHIP, DIM), F32),
            vm((NCHIP, DIM, TOK), F32), vm((NCHIP, DIM, TOK), F32),
            vm((NCHIP, 1, TOK), F32), vm((NCHIP, NCHIP, 1, TOK), F32), vm((NCHIP, 1, TOK), F32),
            vm((TV, NT), F32), vm((TV, NT), F32), vm((TV, NT), BF16), vm((TV, NT), BF16),
        ]
        + eight + one + [dma((NCHIP, NCHIP))] * 2 + eight + one,
        compiler_params=params(4, 63),
    )(hn, table, lab, coef)


def rms_scale(rows_wide, norm_gain):
    inv_rms = lax.rsqrt(jnp.mean(rows_wide * rows_wide, axis=-1, keepdims=True) + NORM_EPS)
    return (rows_wide * inv_rms * norm_gain).astype(BF16), inv_rms


def rms_back(rows_wide, inv_rms, norm_gain, grad_out):
    scaled_grad = grad_out * norm_gain
    return inv_rms * (scaled_grad - rows_wide * (inv_rms * inv_rms) * jnp.mean(scaled_grad * rows_wide, axis=-1, keepdims=True))


def solution(mesh):
    def device_step(tok_ids, tok_labels, loss_mask, table, gain_mlp, gain_head, gate_shard, up_shard, down_shard):
        meta = jnp.stack([tok_ids, tok_labels, loss_mask])[:, None, :]
        gains = (gain_mlp[None], gain_head[None])
        ids_all, lab_rel, coef, pos, full, emb_rows, local, *acts, gate_full, up_full, down_full = start(meta, gate_shard, up_shard, down_shard, table, *gains)

        devices = jnp.arange(NDEV, dtype=jnp.int32)
        rounds = (full[0, 0] + CAP - 1) // CAP
        slots = jnp.arange(NDEV * CAP, dtype=jnp.int32)

        def places(ids_all, tok_ids):
            upper = jnp.triu(jnp.ones((TOK, TOK), BF16), 1)
            lids = ids_all - lax.axis_index("fsdp") * ROWS
            owned = (lids >= 0) & (lids < ROWS)
            key = jnp.where(owned, jnp.dot(owned.astype(BF16), upper, preferred_element_type=F32).astype(jnp.int32), -1)
            owner = tok_ids // ROWS
            is_owner = owner[None, :] == devices[:, None]
            my_rank = jnp.sum(jnp.where(is_owner, jnp.dot(is_owner.astype(BF16), upper, preferred_element_type=F32), 0.0), axis=0).astype(jnp.int32)

            def place(r):
                slot = my_rank - r * CAP
                return jnp.where((slot >= 0) & (slot < CAP), owner * CAP + slot, -1)

            return lids, key, place

        def more_rows(rows, acts, ids_all, tok_ids, table):
            lids, key, place = places(ids_all, tok_ids)

            def one(r, rows):
                got, _ = fetch_rows(key - r * CAP, lids, table)
                pick = (place(r)[:, None] == slots[None, :]).astype(BF16)
                return rows + jnp.dot(pick, got.reshape(NDEV * CAP, DIM), preferred_element_type=F32).astype(BF16)

            rows = lax.fori_loop(1, rounds, one, rows)
            return rows, tuple(forward_again(rows, *gains, gate_full, up_full, down_full))

        emb_rows, acts = lax.cond(rounds > 1, more_rows, lambda rows, acts, *_: (rows, acts), emb_rows, tuple(acts), ids_all, tok_ids, table)
        hid, h_norm = acts
        d_hnorm_t, head_grad, loss_part = head(h_norm, table, lab_rel, coef)
        where = local.reshape(1, NDEV * CAP).astype(jnp.int32)
        grad_table, out_gate, out_up, out_down, loss, grad_x = finish(
            pos, d_hnorm_t, emb_rows, hid, gate_full, up_full, down_full, *gains, where, head_grad, loss_part
        )

        def more_grads(acc, ids_all, tok_ids, grad_x):
            lids, key, place = places(ids_all, tok_ids)

            def one(r, acc):
                got = send_grads(place(r)[None], grad_x)
                hit = (key - r * CAP)[:, None, :] == jnp.arange(CAP, dtype=jnp.int32)[None, :, None]
                return add_rows(jnp.sum(jnp.where(hit, (lids + 1)[:, None, :], 0), axis=2), got, acc)

            return lax.fori_loop(1, rounds, one, acc)

        grad_table = lax.cond(rounds > 1, more_grads, lambda acc, *_: acc, grad_table, ids_all, tok_ids, grad_x)
        return loss[0, 0], grad_table, out_gate, out_up, out_down

    row_spec = P("fsdp", None)
    tok_spec = P("fsdp")
    return jax.shard_map(device_step, mesh=mesh, in_specs=(tok_spec, tok_spec, tok_spec, row_spec, P(), P(), row_spec, row_spec, row_spec), out_specs=(P(), row_spec, row_spec, row_spec, row_spec), check_vma=False)
```
